128 devices in a mesh: blk: 32 (over z, x, core), rows: 4 (over y).
Axes of the slice: x: 4, y: 4, z: 4, core: 2. Of those that a mesh axis runs over, the one named last changes fastest.
Arguments:
- columns: float32 [2048, 16384], P('blk', 'rows'), may hold values from -100 to 100
- plan: int32 [3, 64], replicated, may hold values from 0 to 63, as said below
Outputs:
- swept: float32 [2048, 16384], P('blk', 'rows')
- off_ratio: float32 [3], replicated
The draws below stay inside these ranges and needn't reach their ends.
Inputs may be any that keep to these rules, and one draw needn't show every extreme that they name: `plan`: row s is a permutation of the 64 positions (position k is slot k % 2 of blk index k // 2). In each row there are a slot t and a number m of 1 to 31 such that the block in slot t of every blk index i goes to slot t of blk index (i + m) modulo 64 / 2, and every other block stays where it is.
All inputs are finite; a program needn't handle non-finite values. Where the reference program divides by a largest or mean magnitude, that divisor is 1e-20 or more.
Results may differ from the reference program's by a relative error of at most 0.00011.
Values sent between devices are 32-bit elements; how exact they have to be, the bound alone decides.
A program may use at most 64 MiB of HBM per device.

```python
import math
import jax
import jax.numpy as jnp
from jax import lax

BW = 32
STEPS = 3
EIG_ITERS = 3
NS_ITERS = 8
BLOCKS = 64
NCOL = 2048
M = 16384


def draw_columns(key, part):
    keys = jax.random.split(jax.random.fold_in(key, 11), 2)
    position = jnp.arange(NCOL, dtype=jnp.float32) / NCOL
    scales = jnp.exp(jax.random.uniform(keys[0], (NCOL,), jnp.float32, 0.0, math.log(6.0)))
    entries = jax.random.normal(keys[1], (NCOL, M), jnp.float32)
    trend = 1.0 + 0.8 * position
    values = entries * (scales * trend)[:, None]
    return jnp.clip(values, -100.0, 100.0).astype(jnp.float32)


def draw_plan(key, part):
    keys = jax.random.split(jax.random.fold_in(key, 23), 2)
    half = BLOCKS // 2
    partner_steps = jax.random.randint(keys[0], (STEPS,), 1, half)
    leaving_slots = jax.random.randint(keys[1], (STEPS,), 0, 2)
    position = jnp.arange(BLOCKS, dtype=jnp.int32)
    device_index = position // 2
    slot_index = position % 2
    moved = (device_index[None, :] + partner_steps[:, None]) % half * 2 + slot_index[None, :]
    table = jnp.where(slot_index[None, :] == leaving_slots[:, None], moved, position[None, :])
    return table.astype(jnp.int32)


def setup_inputs(seed: int = 0) -> dict:
    key_of = jax.random.split(jax.random.key(seed), 3)
    return {
        "columns": draw_columns(jax.random.fold_in(key_of[2], 71), 0),
        "plan": draw_plan(jax.random.fold_in(key_of[2], 71), 0),
    }


PRECISE = lax.Precision.HIGHEST

def matmul(left, right):
    return jnp.matmul(left, right, precision=PRECISE, preferred_element_type=jnp.float32)

def flipped(matrix):
    return jnp.swapaxes(matrix, -1, -2)

def orthonormal(matrix):
    lengths = jnp.sqrt(lax.optimization_barrier(jnp.sum(matrix * matrix, axis=-2, keepdims=True)))
    normed = matrix / lengths
    inner = matmul(flipped(normed), normed)
    bound = lax.optimization_barrier(jnp.max(lax.optimization_barrier(jnp.sum(jnp.abs(inner), axis=-1)), axis=-1))
    normed = normed / jnp.sqrt(bound)[..., None, None]
    for turn_index in range(NS_ITERS):
        normed = 1.5 * normed - 0.5 * matmul(normed, matmul(flipped(normed), normed))
    return normed

def pair_rotation(gram_sum):
    rotation = jnp.broadcast_to(jnp.eye(gram_sum.shape[-1], dtype=gram_sum.dtype), gram_sum.shape)
    for turn_index in range(EIG_ITERS):
        rotation = orthonormal(matmul(gram_sum, rotation))
    return rotation

def reference(columns, plan):
    current = columns
    eye_mask = jnp.eye(2 * BW, dtype=bool)
    ratios = []
    for step_index in range(STEPS):
        pairs = current.reshape(BLOCKS // 2, 2 * BW, M)
        gram_sum = matmul(pairs, flipped(pairs))
        off_part = jnp.where(eye_mask, 0.0, gram_sum)
        diag_part = jnp.where(eye_mask, gram_sum, 0.0)
        off_total = jnp.sum(off_part * off_part)
        diag_total = jnp.sum(diag_part * diag_part)
        ratios.append(jnp.sqrt(off_total) / jnp.sqrt(diag_total))
        rotation = pair_rotation(gram_sum)
        rotated = matmul(flipped(rotation), pairs)
        blocks = rotated.reshape(BLOCKS, BW, M)
        placed = jnp.zeros_like(blocks).at[plan[step_index]].set(blocks)
        current = placed.reshape(NCOL, M)
    return (current, jnp.stack(ratios))
```

```python
from functools import partial

import jax
import jax.numpy as jnp
from jax import lax
from jax.experimental import pallas as pl
from jax.experimental.pallas import tpu as pltpu
from jax.sharding import PartitionSpec as P

STEPS = 3
EIG_ITERS = 3
NS_ITERS = 8
F32 = jnp.float32
BF16 = jnp.bfloat16
NT = (((1,), (1,)), ((), ()))
MESH = pl.DeviceIdType.MESH


def dot(left, right):
    return jnp.dot(left, right, preferred_element_type=F32)


def left_mask(shape):
    return lax.broadcasted_iota(jnp.int32, shape, 1) < shape[1] // 2


def parts(wide):
    high = wide.astype(BF16)
    rest = wide - high.astype(F32)
    middle = rest.astype(BF16)
    last = rest - middle.astype(F32)
    return high, rest, middle, last


def as_left(twice):
    high, rest, middle, last = parts(twice)
    mask = left_mask(twice.shape)
    first = jnp.where(mask, twice, rest).astype(BF16)
    second = jnp.where(mask, twice, last).astype(BF16)
    return jnp.concatenate([first, first, second], axis=1)


def as_right(wide):
    high, rest, middle, last = parts(wide)
    return jnp.concatenate([high, high, middle, middle, last.astype(BF16), high], axis=0)


def as_right_transposed(twice):
    high, rest, middle, last = parts(twice)
    mask = left_mask(twice.shape)
    third = jnp.where(mask, last, twice).astype(BF16)
    rows = jnp.concatenate([high, middle, third], axis=1)
    return jnp.concatenate([rows, rows], axis=0)


def rotation_rows(gram):
    size = gram.shape[0]
    shape = gram.shape
    row = lax.broadcasted_iota(jnp.int32, shape, 0)
    column = lax.broadcasted_iota(jnp.int32, shape, 1)
    diagonal = (column == row) | (column == row + size)
    eye = jnp.where(diagonal, 1.0, 0.0).astype(F32)
    left = left_mask(shape)
    gram_right = as_right(gram)

    def turn(index, carry):
        z = carry
        z_left = as_left(z)
        inner = lax.dot_general(z_left, as_right_transposed(z), NT, preferred_element_type=F32)
        z_gram = dot(z_left, gram_right)
        squares = jnp.where(diagonal, inner, 0.0)
        scale_row = lax.rsqrt(jnp.sum(squares, axis=0, keepdims=True))
        scale_column = lax.rsqrt(0.5 * jnp.sum(squares, axis=1, keepdims=True))
        inner = inner * scale_column * scale_row
        bound = jnp.max(jnp.sum(jnp.abs(inner), axis=0, keepdims=True), axis=1, keepdims=True)
        x = eye - inner / bound
        both = jnp.where(left, z_gram, z) * (scale_column * lax.rsqrt(bound))
        total = eye + 0.5 * x
        for step in range(NS_ITERS - 1):
            x_right = as_right(x)
            if step == 0:
                square = dot(as_left(x), x_right)
            else:
                stacked = dot(jnp.concatenate([as_left(x), as_left(total)], axis=0), x_right)
                square = stacked[:size]
                total = total + 0.5 * stacked[size:]
            x = 0.75 * square + 0.25 * dot(as_left(square), x_right)
        both = dot(as_left(total), as_right(both))
        both = both + 0.5 * dot(as_left(x), as_right(both))
        other = pltpu.roll(both, size, 1)
        last = index == EIG_ITERS - 1
        return jnp.where(left == jnp.logical_not(last), both, other)

    return lax.fori_loop(0, EIG_ITERS, turn, gram)


def step_kernel(first_ref, second_ref, flag_ref, stay_ref, move_ref, sums_ref, grams, send_sem, recv_sem):
    me = lax.axis_index("rows")
    count = lax.axis_size("rows")
    barrier = pltpu.get_barrier_semaphore()
    for away in range(1, count):
        peer = lax.rem(me + away, count)
        pl.semaphore_signal(barrier, inc=1, device_id={"rows": peer}, device_id_type=MESH)

    width = first_ref.shape[0]
    size = 2 * width
    columns = first_ref.shape[1]

    current = jnp.concatenate([first_ref[...], second_ref[...]], axis=0)
    high = current.astype(BF16)
    low = (current - high.astype(F32)).astype(BF16)
    pieces = jnp.concatenate([high, low], axis=0)
    products = lax.dot_general(pieces, pieces, NT, preferred_element_type=F32)
    products = products[:size] + products[size:]
    grams[me] = products + pltpu.roll(products, size, 1)

    pl.semaphore_wait(barrier, count - 1)
    copies = []
    for away in range(1, count):
        peer = lax.rem(me + away, count)
        copy = pltpu.make_async_remote_copy(
            src_ref=grams.at[me],
            dst_ref=grams.at[me],
            send_sem=send_sem.at[away - 1],
            recv_sem=recv_sem.at[away - 1],
            device_id={"rows": peer},
            device_id_type=MESH,
        )
        copy.start()
        copies.append(copy)
    for copy in copies:
        copy.wait()
    gram = (grams[0] + grams[1]) + (grams[2] + grams[3])

    row = lax.broadcasted_iota(jnp.int32, gram.shape, 0)
    column = lax.broadcasted_iota(jnp.int32, gram.shape, 1)
    squares = jnp.where(column < size, gram * gram, 0.0)
    off = jnp.sum(jnp.where(column == row, 0.0, squares), axis=0, keepdims=True)
    diag = jnp.sum(jnp.where(column == row, squares, 0.0), axis=0, keepdims=True)
    sums_ref[...] = jnp.concatenate([off, diag], axis=0)

    rotation = rotation_rows(gram)
    flag = flag_ref[...]
    top, bottom = rotation[:width], rotation[width:]
    ordered = jnp.concatenate(
        [flag * bottom + (1.0 - flag) * top, flag * top + (1.0 - flag) * bottom], axis=0
    )
    rest = ordered - ordered.astype(BF16).astype(F32)
    mask = left_mask(ordered.shape)
    first = jnp.where(mask, ordered, rest).astype(BF16)
    weights = jnp.concatenate([first, ordered.astype(BF16)], axis=1)[:, : 3 * size]
    rotated = dot(weights, jnp.concatenate([high, high, low], axis=0))
    stay_ref[...] = rotated[:width]
    move_ref[...] = rotated[width:]


def step(first, second, flag):
    whole = first is second
    width = first.shape[0] // 2 if whole else first.shape[0]
    columns = first.shape[1]
    block = (width, columns)
    size = 2 * width
    return pl.pallas_call(
        step_kernel,
        grid=(1,),
        out_shape=(
            jax.ShapeDtypeStruct(block, F32),
            jax.ShapeDtypeStruct(block, F32),
            jax.ShapeDtypeStruct((2, 2 * size), F32),
        ),
        in_specs=[
            pl.BlockSpec(block, lambda i: (0, 0)),
            pl.BlockSpec(block, lambda i: (1 if whole else 0, 0)),
            pl.BlockSpec((1, 2 * size), lambda i: (0, 0)),
        ],
        out_specs=(
            pl.BlockSpec(block, lambda i: (0, 0)),
            pl.BlockSpec(block, lambda i: (0, 0)),
            pl.BlockSpec((2, 2 * size), lambda i: (0, 0)),
        ),
        scratch_shapes=[
            pltpu.VMEM((4, size, 2 * size), F32),
            pltpu.SemaphoreType.DMA((3,)),
            pltpu.SemaphoreType.DMA((3,)),
        ],
        compiler_params=pltpu.CompilerParams(
            collective_id=1 if whole else 2, has_side_effects=True, vmem_limit_bytes=40 * 1024 * 1024
        ),
        name="first_step" if whole else "later_step",
    )(first, second, flag)


def move_by(values, distance):
    count = lax.axis_size("blk")
    return lax.ppermute(values, "blk", [(k, (k + distance) % count) for k in range(count)])


def local(columns, plan):
    cycle = lax.axis_size("blk")
    branches = [partial(move_by, distance=distance) for distance in range(1, cycle)]
    first_slot = jnp.int32(0)
    first, second = columns, columns
    sums = []
    for index in range(STEPS):
        leaving = (plan[index, 1] != 1).astype(jnp.int32)
        distance = jnp.maximum(plan[index, 0] // 2, plan[index, 1] // 2)
        flag = jnp.broadcast_to((leaving == first_slot).astype(F32), (1, 128))
        stay, move, part = step(first, second, flag)
        sums.append(part)
        first, second = stay, lax.switch(distance - 1, branches, move)
        first_slot = 1 - leaving
    swept = jnp.where(
        first_slot == 0,
        jnp.concatenate([first, second], axis=0),
        jnp.concatenate([second, first], axis=0),
    )
    flat = jnp.sum(jnp.stack(sums), axis=2).reshape(1, 2 * STEPS)
    gathered = lax.all_to_all(jnp.broadcast_to(flat, (cycle, 2 * STEPS)), "blk", 0, 0, tiled=True)
    totals = jnp.sum(gathered, axis=0).reshape(STEPS, 2)
    return swept, jnp.sqrt(totals[:, 0]) / jnp.sqrt(totals[:, 1])


def solution(mesh):
    return jax.shard_map(
        local,
        mesh=mesh,
        in_specs=(P("blk", "rows"), P()),
        out_specs=(P("blk", "rows"), P()),
        check_vma=False,
    )
```

```python
from functools import partial

import jax
import jax.numpy as jnp
from jax import lax
from jax.experimental import pallas as pl
from jax.experimental.pallas import tpu as pltpu
from jax.sharding import PartitionSpec as P

STEPS = 3
EIG_ITERS = 3
NS_ITERS = 8
F32 = jnp.float32
BF16 = jnp.bfloat16
NT = (((1,), (1,)), ((), ()))
MESH = pl.DeviceIdType.MESH


def dot(left, right):
    return jnp.dot(left, right, preferred_element_type=F32)


def left_mask(shape):
    return lax.broadcasted_iota(jnp.int32, shape, 1) < shape[1] // 2


def parts(wide):
    high = wide.astype(BF16)
    rest = wide - high.astype(F32)
    middle = rest.astype(BF16)
    last = rest - middle.astype(F32)
    return high, rest, middle, last


def as_left(twice):
    high, rest, middle, last = parts(twice)
    mask = left_mask(twice.shape)
    first = jnp.where(mask, twice, rest).astype(BF16)
    second = jnp.where(mask, twice, last).astype(BF16)
    return jnp.concatenate([first, first, second], axis=1)


def as_right(wide):
    high, rest, middle, last = parts(wide)
    return jnp.concatenate([high, high, middle, middle, last.astype(BF16), high], axis=0)


def as_right_transposed(twice):
    high, rest, middle, last = parts(twice)
    mask = left_mask(twice.shape)
    third = jnp.where(mask, last, twice).astype(BF16)
    rows = jnp.concatenate([high, middle, third], axis=1)
    return jnp.concatenate([rows, rows], axis=0)


def rotation_rows(gram):
    size = gram.shape[0]
    shape = gram.shape
    row = lax.broadcasted_iota(jnp.int32, shape, 0)
    column = lax.broadcasted_iota(jnp.int32, shape, 1)
    diagonal = (column == row) | (column == row + size)
    eye = jnp.where(diagonal, 1.0, 0.0).astype(F32)
    left = left_mask(shape)
    gram_right = as_right(gram)

    def turn(index, carry):
        z = carry
        z_left = as_left(z)
        inner = lax.dot_general(z_left, as_right_transposed(z), NT, preferred_element_type=F32)
        z_gram = dot(z_left, gram_right)
        squares = jnp.where(diagonal, inner, 0.0)
        scale_row = lax.rsqrt(jnp.sum(squares, axis=0, keepdims=True))
        scale_column = lax.rsqrt(0.5 * jnp.sum(squares, axis=1, keepdims=True))
        inner = inner * scale_column * scale_row
        bound = jnp.max(jnp.sum(jnp.abs(inner), axis=0, keepdims=True), axis=1, keepdims=True)
        x = eye - inner / bound
        both = jnp.where(left, z_gram, z) * (scale_column * lax.rsqrt(bound))
        total = eye + 0.5 * x
        for step in range(NS_ITERS - 1):
            x_right = as_right(x)
            if step == 0:
                square = dot(as_left(x), x_right)
            else:
                stacked = dot(jnp.concatenate([as_left(x), as_left(total)], axis=0), x_right)
                square = stacked[:size]
                total = total + 0.5 * stacked[size:]
            x = 0.75 * square + 0.25 * dot(as_left(square), x_right)
        both = dot(as_left(total), as_right(both))
        both = both + 0.5 * dot(as_left(x), as_right(both))
        other = pltpu.roll(both, size, 1)
        last = index == EIG_ITERS - 1
        return jnp.where(left == jnp.logical_not(last), both, other)

    return lax.fori_loop(0, EIG_ITERS, turn, gram)


def step_kernel(first_ref, second_ref, flag_ref, stay_ref, move_ref, sums_ref, grams, send_sem, recv_sem):
    me = lax.axis_index("rows")
    count = lax.axis_size("rows")
    barrier = pltpu.get_barrier_semaphore()
    for away in range(1, count):
        peer = lax.rem(me + away, count)
        pl.semaphore_signal(barrier, inc=1, device_id={"rows": peer}, device_id_type=MESH)

    width = first_ref.shape[0]
    size = 2 * width
    columns = first_ref.shape[1]

    current = jnp.concatenate([first_ref[...], second_ref[...]], axis=0)
    high = current.astype(BF16)
    low = (current - high.astype(F32)).astype(BF16)
    pieces = jnp.concatenate([high, low], axis=0)
    products = lax.dot_general(pieces, pieces, NT, preferred_element_type=F32)
    products = products[:size] + products[size:]
    grams[me] = products + pltpu.roll(products, size, 1)

    pl.semaphore_wait(barrier, count - 1)
    copies = []
    for away in range(1, count):
        peer = lax.rem(me + away, count)
        copy = pltpu.make_async_remote_copy(
            src_ref=grams.at[me],
            dst_ref=grams.at[me],
            send_sem=send_sem.at[away - 1],
            recv_sem=recv_sem.at[away - 1],
            device_id={"rows": peer},
            device_id_type=MESH,
        )
        copy.start()
        copies.append(copy)
    for copy in copies:
        copy.wait()
    gram = (grams[0] + grams[1]) + (grams[2] + grams[3])

    row = lax.broadcasted_iota(jnp.int32, gram.shape, 0)
    column = lax.broadcasted_iota(jnp.int32, gram.shape, 1)
    squares = jnp.where(column < size, gram * gram, 0.0)
    off = jnp.sum(jnp.where(column == row, 0.0, squares), axis=0, keepdims=True)
    diag = jnp.sum(jnp.where(column == row, squares, 0.0), axis=0, keepdims=True)
    sums_ref[...] = jnp.concatenate([off, diag], axis=0)

    rotation = rotation_rows(gram)
    flag = flag_ref[...]
    top, bottom = rotation[:width], rotation[width:]
    ordered = jnp.concatenate(
        [flag * bottom + (1.0 - flag) * top, flag * top + (1.0 - flag) * bottom], axis=0
    )
    rest = ordered - ordered.astype(BF16).astype(F32)
    mask = left_mask(ordered.shape)
    first = jnp.where(mask, ordered, rest).astype(BF16)
    weights = jnp.concatenate([first, ordered.astype(BF16)], axis=1)[:, : 3 * size]
    rotated = dot(weights, jnp.concatenate([high, high, low], axis=0))
    stay_ref[...] = rotated[:width]
    move_ref[...] = rotated[width:]


def step(first, second, flag):
    whole = first is second
    width = first.shape[0] // 2 if whole else first.shape[0]
    columns = first.shape[1]
    block = (width, columns)
    size = 2 * width
    return pl.pallas_call(
        step_kernel,
        grid=(1,),
        out_shape=(
            jax.ShapeDtypeStruct(block, F32),
            jax.ShapeDtypeStruct(block, F32),
            jax.ShapeDtypeStruct((2, 2 * size), F32),
        ),
        in_specs=[
            pl.BlockSpec(block, lambda i: (0, 0)),
            pl.BlockSpec(block, lambda i: (1 if whole else 0, 0)),
            pl.BlockSpec((1, 2 * size), lambda i: (0, 0)),
        ],
        out_specs=(
            pl.BlockSpec(block, lambda i: (0, 0)),
            pl.BlockSpec(block, lambda i: (0, 0)),
            pl.BlockSpec((2, 2 * size), lambda i: (0, 0)),
        ),
        scratch_shapes=[
            pltpu.VMEM((4, size, 2 * size), F32),
            pltpu.SemaphoreType.DMA((3,)),
            pltpu.SemaphoreType.DMA((3,)),
        ],
        compiler_params=pltpu.CompilerParams(
            collective_id=1 if whole else 2, has_side_effects=True, vmem_limit_bytes=40 * 1024 * 1024
        ),
        name="first_step" if whole else "later_step",
    )(first, second, flag)


def shift_kernel(distance, values_ref, moved_ref, send_sem, recv_sem):
    me = lax.axis_index("blk")
    count = lax.axis_size("blk")
    target = lax.rem(me + distance, count)
    origin = lax.rem(me + (count - distance), count)
    barrier = pltpu.get_barrier_semaphore()
    pl.semaphore_signal(barrier, inc=1, device_id={"blk": origin}, device_id_type=MESH)
    pl.semaphore_wait(barrier, 1)
    copy = pltpu.make_async_remote_copy(
        src_ref=values_ref,
        dst_ref=moved_ref,
        send_sem=send_sem,
        recv_sem=recv_sem,
        device_id={"blk": target},
        device_id_type=MESH,
    )
    copy.start()
    copy.wait()


def move_by(values, distance):
    return pl.pallas_call(
        partial(shift_kernel, distance),
        out_shape=jax.ShapeDtypeStruct(values.shape, values.dtype),
        in_specs=[pl.BlockSpec(memory_space=pltpu.VMEM)],
        out_specs=pl.BlockSpec(memory_space=pltpu.VMEM),
        scratch_shapes=[pltpu.SemaphoreType.DMA, pltpu.SemaphoreType.DMA],
        compiler_params=pltpu.CompilerParams(collective_id=2 + distance, has_side_effects=True),
        name=f"shift_{distance}",
    )(values)


def plan_kernel(plan_ref, first_ref, second_ref, third_ref, flags_ref):
    slot = jnp.int32(0)
    for index, branch_ref in enumerate((first_ref, second_ref, third_ref)):
        stays = (plan_ref[index, 1] == 1).astype(jnp.int32)
        branch_ref[0] = jnp.maximum(plan_ref[index, 0] >> 1, plan_ref[index, 1] >> 1) - 1
        leaves = ((1 - stays) == slot).astype(F32)
        flags_ref[index] = jnp.full((1, 128), leaves, F32)
        slot = stays
    flags_ref[STEPS] = jnp.full((1, 128), slot.astype(F32), F32)


def read_plan(plan):
    one = jax.ShapeDtypeStruct((1,), jnp.int32)
    smem = pl.BlockSpec(memory_space=pltpu.SMEM)
    return pl.pallas_call(
        plan_kernel,
        out_shape=(one, one, one, jax.ShapeDtypeStruct((STEPS + 1, 1, 128), F32)),
        in_specs=[smem],
        out_specs=(smem, smem, smem, pl.BlockSpec(memory_space=pltpu.VMEM)),
        name="read_plan",
    )(plan)


def local(columns, plan):
    cycle = lax.axis_size("blk")
    branches = [partial(move_by, distance=distance) for distance in range(1, cycle)]
    *chosen, flags = read_plan(plan)
    first, second = columns, columns
    sums = []
    for index in range(STEPS):
        stay, move, part = step(first, second, flags[index])
        sums.append(part)
        first, second = stay, lax.switch(chosen[index][0], branches, move)
    swap = flags[STEPS, 0, :1] != 0.0
    swept = jnp.where(
        swap[:, None],
        jnp.concatenate([second, first], axis=0),
        jnp.concatenate([first, second], axis=0),
    )
    flat = jnp.sum(jnp.stack(sums), axis=2).reshape(1, 2 * STEPS)
    gathered = lax.all_to_all(jnp.broadcast_to(flat, (cycle, 2 * STEPS)), "blk", 0, 0, tiled=True)
    totals = jnp.sum(gathered, axis=0).reshape(STEPS, 2)
    return swept, jnp.sqrt(totals[:, 0]) / jnp.sqrt(totals[:, 1])


def solution(mesh):
    return jax.shard_map(
        local,
        mesh=mesh,
        in_specs=(P("blk", "rows"), P()),
        out_specs=(P("blk", "rows"), P()),
        check_vma=False,
    )
```

```python
from functools import partial

import jax
import jax.numpy as jnp
from jax import lax
from jax.experimental import pallas as pl
from jax.experimental.pallas import tpu as pltpu
from jax.sharding import PartitionSpec as P

STEPS = 3
EIG_ITERS = 3
NS_ITERS = 8
F32 = jnp.float32
BF16 = jnp.bfloat16
NT = (((1,), (1,)), ((), ()))
MESH = pl.DeviceIdType.MESH


def dot(left, right):
    return jnp.dot(left, right, preferred_element_type=F32)


def left_mask(shape):
    return lax.broadcasted_iota(jnp.int32, shape, 1) < shape[1] // 2


def parts(wide):
    high = wide.astype(BF16)
    rest = wide - high.astype(F32)
    middle = rest.astype(BF16)
    last = rest - middle.astype(F32)
    return high, rest, middle, last


def as_left(twice):
    high, rest, middle, last = parts(twice)
    mask = left_mask(twice.shape)
    first = jnp.where(mask, twice, rest).astype(BF16)
    second = jnp.where(mask, twice, last).astype(BF16)
    return jnp.concatenate([first, first, second], axis=1)


def as_right(wide):
    high, rest, middle, last = parts(wide)
    return jnp.concatenate([high, high, middle, middle, last.astype(BF16), high], axis=0)


def as_right_transposed(twice):
    high, rest, middle, last = parts(twice)
    mask = left_mask(twice.shape)
    third = jnp.where(mask, last, twice).astype(BF16)
    rows = jnp.concatenate([high, middle, third], axis=1)
    return jnp.concatenate([rows, rows], axis=0)


def rotation_rows(gram):
    size = gram.shape[0]
    shape = gram.shape
    row = lax.broadcasted_iota(jnp.int32, shape, 0)
    column = lax.broadcasted_iota(jnp.int32, shape, 1)
    diagonal = (column == row) | (column == row + size)
    eye = jnp.where(diagonal, 1.0, 0.0).astype(F32)
    left = left_mask(shape)
    gram_right = as_right(gram)

    def polar_turn(step, carry):
        x, total = carry
        x_right = as_right(x)
        stacked = dot(jnp.concatenate([as_left(x), as_left(total)], axis=0), x_right)
        square = stacked[:size]
        total = total + 0.5 * stacked[size:]
        return 0.75 * square + 0.25 * dot(as_left(square), x_right), total

    def turn(index, z):
        z_left = as_left(z)
        inner = lax.dot_general(z_left, as_right_transposed(z), NT, preferred_element_type=F32)
        z_gram = dot(z_left, gram_right)
        squares = jnp.where(diagonal, inner, 0.0)
        scale_row = lax.rsqrt(jnp.sum(squares, axis=0, keepdims=True))
        scale_column = lax.rsqrt(0.5 * jnp.sum(squares, axis=1, keepdims=True))
        inner = inner * scale_column * scale_row
        bound = jnp.max(jnp.sum(jnp.abs(inner), axis=0, keepdims=True), axis=1, keepdims=True)
        x = eye - inner / bound
        both = jnp.where(left, z_gram, z) * (scale_column * lax.rsqrt(bound))
        x, total = lax.fori_loop(0, NS_ITERS - 1, polar_turn, (x, eye))
        both = dot(as_left(total), as_right(both))
        both = both + 0.5 * dot(as_left(x), as_right(both))
        other = pltpu.roll(both, size, 1)
        last = index == EIG_ITERS - 1
        return jnp.where(left == jnp.logical_not(last), both, other)

    return lax.fori_loop(0, EIG_ITERS, turn, gram)


def two_parts(values):
    high = values.astype(BF16)
    return high, (values - high.astype(F32)).astype(BF16)


def left_of_three(twice):
    rest = twice - twice.astype(BF16).astype(F32)
    first = jnp.where(left_mask(twice.shape), twice, rest).astype(BF16)
    return jnp.concatenate([first, twice.astype(BF16)], axis=1)[:, : 3 * twice.shape[1] // 2]


def right_of_three(values):
    high, low = two_parts(values)
    return jnp.concatenate([high, high, low], axis=0)


RAW = 1536
TILE = 512
GRAM_TILE = 1024


def at_tile(index, tile, start=0):
    return pl.ds(pl.multiple_of(start + index * tile, 128), tile)


def step_kernel(
    distance, first_ref, second_ref, flag_ref, stay_ref, come_ref, sums_ref,
    grams, raw_first, raw_second, rows_out, rows_in, move_out,
    gram_send, gram_recv, raw_send, raw_recv, rows_send, rows_recv, move_send, move_recv,
):
    me = lax.axis_index("rows")
    count = lax.axis_size("rows")
    here = lax.axis_index("blk")
    cycle = lax.axis_size("blk")
    target = lax.rem(here + distance, cycle)
    origin = lax.rem(here + (cycle - distance), cycle)
    width, columns = first_ref.shape
    size = 2 * width

    barrier = pltpu.get_barrier_semaphore()
    for away in range(1, count):
        peer = lax.rem(me + away, count)
        pl.semaphore_signal(barrier, inc=1, device_id={"rows": peer}, device_id_type=MESH)
    pl.semaphore_signal(barrier, inc=1, device_id={"blk": origin}, device_id_type=MESH)

    def to_target(source, destination, send_sem, recv_sem):
        return pltpu.make_async_remote_copy(
            src_ref=source, dst_ref=destination, send_sem=send_sem, recv_sem=recv_sem,
            device_id={"blk": target}, device_id_type=MESH,
        )

    def gram_tile(index, total):
        tile = at_tile(index, GRAM_TILE)
        current = jnp.concatenate([first_ref[:, tile], second_ref[:, tile]], axis=0)
        pieces = jnp.concatenate(two_parts(current), axis=0)
        return total + lax.dot_general(pieces, pieces, NT, preferred_element_type=F32)

    products = lax.fori_loop(0, columns // GRAM_TILE, gram_tile, jnp.zeros((2 * size, 2 * size), F32))
    products = products[:size] + products[size:]
    grams[me] = products + pltpu.roll(products, size, 1)

    pl.semaphore_wait(barrier, count)
    copies = []
    for away in range(1, count):
        peer = lax.rem(me + away, count)
        copy = pltpu.make_async_remote_copy(
            src_ref=grams.at[me], dst_ref=grams.at[me],
            send_sem=gram_send.at[away - 1], recv_sem=gram_recv.at[away - 1],
            device_id={"rows": peer}, device_id_type=MESH,
        )
        copy.start()
        copies.append(copy)
    raw = [
        to_target(first_ref.at[:, pl.ds(0, RAW)], raw_first, raw_send.at[0], raw_recv.at[0]),
        to_target(second_ref.at[:, pl.ds(0, RAW)], raw_second, raw_send.at[1], raw_recv.at[1]),
    ]
    for copy in raw:
        copy.start()
    for copy in copies:
        copy.wait()
    gram = (grams[0] + grams[1]) + (grams[2] + grams[3])

    row = lax.broadcasted_iota(jnp.int32, gram.shape, 0)
    column = lax.broadcasted_iota(jnp.int32, gram.shape, 1)
    squares = jnp.where(column < size, gram * gram, 0.0)
    off = jnp.sum(jnp.where(column == row, 0.0, squares), axis=0, keepdims=True)
    diag = jnp.sum(jnp.where(column == row, squares, 0.0), axis=0, keepdims=True)
    sums_ref[...] = jnp.concatenate([off, diag], axis=0)

    rotation = rotation_rows(gram)
    flag = flag_ref[...]
    top, bottom = rotation[:width], rotation[width:]
    staying = flag * bottom + (1.0 - flag) * top
    leaving = flag * top + (1.0 - flag) * bottom
    rows_out[...] = leaving
    rows_copy = to_target(rows_out, rows_in, rows_send, rows_recv)
    rows_copy.start()
    weights = left_of_three(jnp.concatenate([staying, leaving], axis=0))

    def move_copy(index):
        return to_target(
            move_out.at[:, at_tile(index, TILE)], come_ref.at[:, at_tile(index, TILE, RAW)],
            move_send.at[index], move_recv.at[index],
        )

    tiles = (columns - RAW) // TILE

    def rotate_tile(index, carry):
        tile = at_tile(index, TILE, RAW)
        current = jnp.concatenate([first_ref[:, tile], second_ref[:, tile]], axis=0)
        rotated = dot(weights, right_of_three(current))
        stay_ref[:, tile] = rotated[:width]
        move_out[:, at_tile(index, TILE)] = rotated[width:]
        move_copy(index).start()
        return carry

    lax.fori_loop(0, tiles, rotate_tile, 0)

    def stay_tile(index, carry):
        tile = at_tile(index, TILE)
        current = jnp.concatenate([first_ref[:, tile], second_ref[:, tile]], axis=0)
        stay_ref[:, tile] = dot(weights[:width], right_of_three(current))
        return carry

    lax.fori_loop(0, RAW // TILE, stay_tile, 0)

    for copy in raw:
        copy.wait()
    rows_copy.wait()
    arrived = left_of_three(rows_in[...])

    def come_tile(index, carry):
        tile = at_tile(index, TILE)
        current = jnp.concatenate([raw_first[:, tile], raw_second[:, tile]], axis=0)
        come_ref[:, tile] = dot(arrived, right_of_three(current))
        return carry

    lax.fori_loop(0, RAW // TILE, come_tile, 0)

    def wait_tile(index, carry):
        move_copy(index).wait()
        return carry

    lax.fori_loop(0, tiles, wait_tile, 0)


def step(first, second, flag, distance):
    width, columns = first.shape
    block = jax.ShapeDtypeStruct((width, columns), F32)
    size = 2 * width
    vmem = pl.BlockSpec(memory_space=pltpu.VMEM)
    tiles = (columns - RAW) // TILE
    dma = pltpu.SemaphoreType.DMA
    return pl.pallas_call(
        partial(step_kernel, distance),
        out_shape=(block, block, jax.ShapeDtypeStruct((2, 2 * size), F32)),
        in_specs=[vmem] * 3,
        out_specs=(vmem,) * 3,
        scratch_shapes=[
            pltpu.VMEM((4, size, 2 * size), F32),
            pltpu.VMEM((width, RAW), F32),
            pltpu.VMEM((width, RAW), F32),
            pltpu.VMEM((width, 2 * size), F32),
            pltpu.VMEM((width, 2 * size), F32),
            pltpu.VMEM((width, columns - RAW), F32),
            dma((3,)), dma((3,)), dma((2,)), dma((2,)), dma, dma, dma((tiles,)), dma((tiles,)),
        ],
        compiler_params=pltpu.CompilerParams(
            collective_id=distance, has_side_effects=True, vmem_limit_bytes=40 * 1024 * 1024
        ),
        name=f"step_{distance}",
    )(first, second, flag)


def plan_kernel(plan_ref, first_ref, second_ref, third_ref, flags_ref):
    slot = jnp.int32(0)
    for index, branch_ref in enumerate((first_ref, second_ref, third_ref)):
        stays = (plan_ref[index, 1] == 1).astype(jnp.int32)
        branch_ref[0] = jnp.maximum(plan_ref[index, 0] >> 1, plan_ref[index, 1] >> 1) - 1
        leaves = ((1 - stays) == slot).astype(F32)
        flags_ref[index] = jnp.full((1, 128), leaves, F32)
        slot = stays
    flags_ref[STEPS] = jnp.full((1, 128), slot.astype(F32), F32)


def read_plan(plan):
    one = jax.ShapeDtypeStruct((1,), jnp.int32)
    smem = pl.BlockSpec(memory_space=pltpu.SMEM)
    return pl.pallas_call(
        plan_kernel,
        out_shape=(one, one, one, jax.ShapeDtypeStruct((STEPS + 1, 1, 128), F32)),
        in_specs=[smem],
        out_specs=(smem, smem, smem, pl.BlockSpec(memory_space=pltpu.VMEM)),
        name="read_plan",
    )(plan)


def local(columns, plan):
    cycle = lax.axis_size("blk")
    width = columns.shape[0] // 2
    branches = [partial(step, distance=distance) for distance in range(1, cycle)]
    *chosen, flags = read_plan(plan)
    first, second = columns[:width], columns[width:]
    sums = []
    for index in range(STEPS):
        first, second, part = lax.switch(chosen[index][0], branches, first, second, flags[index])
        sums.append(part)
    swap = flags[STEPS, 0, :1] != 0.0
    swept = jnp.where(
        swap[:, None],
        jnp.concatenate([second, first], axis=0),
        jnp.concatenate([first, second], axis=0),
    )
    flat = jnp.sum(jnp.stack(sums), axis=2).reshape(1, 2 * STEPS)
    gathered = lax.all_to_all(jnp.broadcast_to(flat, (cycle, 2 * STEPS)), "blk", 0, 0, tiled=True)
    totals = jnp.sum(gathered, axis=0).reshape(STEPS, 2)
    return swept, jnp.sqrt(totals[:, 0]) / jnp.sqrt(totals[:, 1])


def solution(mesh):
    return jax.shard_map(
        local,
        mesh=mesh,
        in_specs=(P("blk", "rows"), P()),
        out_specs=(P("blk", "rows"), P()),
        check_vma=False,
    )
```

```python
from functools import partial

import jax
import jax.numpy as jnp
from jax import lax
from jax.experimental import pallas as pl
from jax.experimental.pallas import tpu as pltpu
from jax.sharding import PartitionSpec as P

STEPS = 3
EIG_ITERS = 3
NS_ITERS = 8
F32 = jnp.float32
BF16 = jnp.bfloat16
NT = (((1,), (1,)), ((), ()))
MESH = pl.DeviceIdType.MESH


def dot(left, right):
    return jnp.dot(left, right, preferred_element_type=F32)


def left_mask(shape):
    return lax.broadcasted_iota(jnp.int32, shape, 1) < shape[1] // 2


def parts(wide):
    high = wide.astype(BF16)
    rest = wide - high.astype(F32)
    middle = rest.astype(BF16)
    last = rest - middle.astype(F32)
    return high, rest, middle, last


def as_left(twice):
    high, rest, middle, last = parts(twice)
    mask = left_mask(twice.shape)
    first = jnp.where(mask, twice, rest).astype(BF16)
    second = jnp.where(mask, twice, last).astype(BF16)
    return jnp.concatenate([first, first, second], axis=1)


def as_right(wide):
    high, rest, middle, last = parts(wide)
    return jnp.concatenate([high, high, middle, middle, last.astype(BF16), high], axis=0)


def as_right_transposed(twice):
    high, rest, middle, last = parts(twice)
    mask = left_mask(twice.shape)
    third = jnp.where(mask, last, twice).astype(BF16)
    rows = jnp.concatenate([high, middle, third], axis=1)
    return jnp.concatenate([rows, rows], axis=0)


def rotation_rows(gram):
    size = gram.shape[0]
    shape = gram.shape
    row = lax.broadcasted_iota(jnp.int32, shape, 0)
    column = lax.broadcasted_iota(jnp.int32, shape, 1)
    diagonal = (column == row) | (column == row + size)
    eye = jnp.where(diagonal, 1.0, 0.0).astype(F32)
    left = left_mask(shape)
    gram_right = as_right(gram)

    def polar_turn(step, carry):
        x, total = carry
        x_right = as_right(x)
        stacked = dot(jnp.concatenate([as_left(x), as_left(total)], axis=0), x_right)
        square = stacked[:size]
        total = total + 0.5 * stacked[size:]
        return 0.75 * square + 0.25 * dot(as_left(square), x_right), total

    def turn(index, z):
        z_left = as_left(z)
        inner = lax.dot_general(z_left, as_right_transposed(z), NT, preferred_element_type=F32)
        z_gram = dot(z_left, gram_right)
        squares = jnp.where(diagonal, inner, 0.0)
        scale_row = lax.rsqrt(jnp.sum(squares, axis=0, keepdims=True))
        scale_column = lax.rsqrt(0.5 * jnp.sum(squares, axis=1, keepdims=True))
        inner = inner * scale_column * scale_row
        bound = jnp.max(jnp.sum(jnp.abs(inner), axis=0, keepdims=True), axis=1, keepdims=True)
        x = eye - inner / bound
        both = jnp.where(left, z_gram, z) * (scale_column * lax.rsqrt(bound))
        x, total = lax.fori_loop(0, NS_ITERS - 1, polar_turn, (x, eye))
        both = dot(as_left(total), as_right(both))
        both = both + 0.5 * dot(as_left(x), as_right(both))
        other = pltpu.roll(both, size, 1)
        last = index == EIG_ITERS - 1
        return jnp.where(left == jnp.logical_not(last), both, other)

    return lax.fori_loop(0, EIG_ITERS, turn, gram)


def two_parts(values):
    high = values.astype(BF16)
    return high, (values - high.astype(F32)).astype(BF16)


def left_of_three(twice):
    rest = twice - twice.astype(BF16).astype(F32)
    first = jnp.where(left_mask(twice.shape), twice, rest).astype(BF16)
    return jnp.concatenate([first, twice.astype(BF16)], axis=1)[:, : 3 * twice.shape[1] // 2]


def right_of_three(values):
    high, low = two_parts(values)
    return jnp.concatenate([high, high, low], axis=0)


NEAR = 8
RAW = 2048
TILE = 512
GRAM_TILE = 1024


def at_tile(index, tile, start=0):
    return pl.ds(pl.multiple_of(start + index * tile, 128), tile)


def step_kernel(
    distance, first_ref, second_ref, flag_ref, stay_ref, come_ref, ratio_ref,
    grams, raw_first, raw_second, rows_out, rows_in, move_out, near_sums, far_sums,
    gram_send, gram_recv, raw_send, raw_recv, rows_send, rows_recv, move_send, move_recv,
    near_send, near_recv, far_send, far_recv,
):
    me = lax.axis_index("rows")
    count = lax.axis_size("rows")
    here = lax.axis_index("blk")
    cycle = lax.axis_size("blk")
    target = lax.rem(here + distance, cycle)
    origin = lax.rem(here + (cycle - distance), cycle)
    width, columns = first_ref.shape
    size = 2 * width

    barrier = pltpu.get_barrier_semaphore()
    for away in range(1, count):
        peer = lax.rem(me + away, count)
        pl.semaphore_signal(barrier, inc=1, device_id={"rows": peer}, device_id_type=MESH)
    near, far = lax.rem(here, NEAR), here // NEAR
    near_peers = [far * NEAR + lax.rem(near + away, NEAR) for away in range(1, NEAR)]
    far_peers = [lax.rem(here + away * NEAR, cycle) for away in range(1, cycle // NEAR)]
    for peer in [origin] + near_peers + far_peers:
        pl.semaphore_signal(barrier, inc=1, device_id={"blk": peer}, device_id_type=MESH)

    def to_peers(peers, buffer, slot, send_sem, recv_sem):
        return [
            pltpu.make_async_remote_copy(
                src_ref=buffer.at[slot], dst_ref=buffer.at[slot],
                send_sem=send_sem.at[index], recv_sem=recv_sem.at[index],
                device_id={"blk": peer}, device_id_type=MESH,
            )
            for index, peer in enumerate(peers)
        ]

    def to_target(source, destination, send_sem, recv_sem):
        return pltpu.make_async_remote_copy(
            src_ref=source, dst_ref=destination, send_sem=send_sem, recv_sem=recv_sem,
            device_id={"blk": target}, device_id_type=MESH,
        )

    def gram_tile(index, total):
        tile = at_tile(index, GRAM_TILE)
        current = jnp.concatenate([first_ref[:, tile], second_ref[:, tile]], axis=0)
        pieces = jnp.concatenate(two_parts(current), axis=0)
        return total + lax.dot_general(pieces, pieces, NT, preferred_element_type=F32)

    products = lax.fori_loop(0, columns // GRAM_TILE, gram_tile, jnp.zeros((2 * size, 2 * size), F32))
    products = products[:size] + products[size:]
    grams[me] = products + pltpu.roll(products, size, 1)

    pl.semaphore_wait(barrier, count + len(near_peers) + len(far_peers))
    copies = []
    for away in range(1, count):
        peer = lax.rem(me + away, count)
        copy = pltpu.make_async_remote_copy(
            src_ref=grams.at[me], dst_ref=grams.at[me],
            send_sem=gram_send.at[away - 1], recv_sem=gram_recv.at[away - 1],
            device_id={"rows": peer}, device_id_type=MESH,
        )
        copy.start()
        copies.append(copy)
    raw = [
        to_target(first_ref.at[:, pl.ds(0, RAW)], raw_first, raw_send.at[0], raw_recv.at[0]),
        to_target(second_ref.at[:, pl.ds(0, RAW)], raw_second, raw_send.at[1], raw_recv.at[1]),
    ]
    for copy in raw:
        copy.start()
    for copy in copies:
        copy.wait()
    gram = (grams[0] + grams[1]) + (grams[2] + grams[3])

    row = lax.broadcasted_iota(jnp.int32, gram.shape, 0)
    column = lax.broadcasted_iota(jnp.int32, gram.shape, 1)
    squares = jnp.where(column < size, gram * gram, 0.0)
    off = jnp.sum(jnp.where(column == row, 0.0, squares), axis=0, keepdims=True)
    diag = jnp.sum(jnp.where(column == row, squares, 0.0), axis=0, keepdims=True)
    near_sums[near] = jnp.concatenate([off, diag, jnp.zeros((6, off.shape[1]), F32)], axis=0)
    near_copies = to_peers(near_peers, near_sums, near, near_send, near_recv)
    for copy in near_copies:
        copy.start()

    rotation = rotation_rows(gram)
    flag = flag_ref[...]
    top, bottom = rotation[:width], rotation[width:]
    staying = flag * bottom + (1.0 - flag) * top
    leaving = flag * top + (1.0 - flag) * bottom
    rows_out[...] = leaving
    rows_copy = to_target(rows_out, rows_in, rows_send, rows_recv)
    rows_copy.start()
    weights = left_of_three(jnp.concatenate([staying, leaving], axis=0))

    def move_copy(index):
        return to_target(
            move_out.at[:, at_tile(index, TILE)], come_ref.at[:, at_tile(index, TILE, RAW)],
            move_send.at[index], move_recv.at[index],
        )

    tiles = (columns - RAW) // TILE

    def rotate_tile(index, carry):
        tile = at_tile(index, TILE, RAW)
        current = jnp.concatenate([first_ref[:, tile], second_ref[:, tile]], axis=0)
        rotated = dot(weights, right_of_three(current))
        stay_ref[:, tile] = rotated[:width]
        move_out[:, at_tile(index, TILE)] = rotated[width:]
        move_copy(index).start()
        return carry

    lax.fori_loop(0, tiles, rotate_tile, 0)

    for copy in near_copies:
        copy.wait()
    far_sums[far] = sum(near_sums[index] for index in range(NEAR))
    far_copies = to_peers(far_peers, far_sums, far, far_send, far_recv)
    for copy in far_copies:
        copy.start()

    def stay_tile(index, carry):
        tile = at_tile(index, TILE)
        current = jnp.concatenate([first_ref[:, tile], second_ref[:, tile]], axis=0)
        stay_ref[:, tile] = dot(weights[:width], right_of_three(current))
        return carry

    lax.fori_loop(0, RAW // TILE, stay_tile, 0)

    for copy in raw:
        copy.wait()
    rows_copy.wait()
    arrived = left_of_three(rows_in[...])

    def come_tile(index, carry):
        tile = at_tile(index, TILE)
        current = jnp.concatenate([raw_first[:, tile], raw_second[:, tile]], axis=0)
        come_ref[:, tile] = dot(arrived, right_of_three(current))
        return carry

    lax.fori_loop(0, RAW // TILE, come_tile, 0)

    def wait_tile(index, carry):
        move_copy(index).wait()
        return carry

    lax.fori_loop(0, tiles, wait_tile, 0)
    for copy in far_copies:
        copy.wait()
    totals = sum(far_sums[index] for index in range(cycle // NEAR))
    roots = jnp.sqrt(jnp.sum(totals[:2], axis=1, keepdims=True))
    ratio_ref[...] = jnp.broadcast_to(roots[:1] / roots[1:], ratio_ref.shape)


def step(first, second, flag, distance):
    width, columns = first.shape
    block = jax.ShapeDtypeStruct((width, columns), F32)
    size = 2 * width
    vmem = pl.BlockSpec(memory_space=pltpu.VMEM)
    tiles = (columns - RAW) // TILE
    dma = pltpu.SemaphoreType.DMA
    return pl.pallas_call(
        partial(step_kernel, distance),
        out_shape=(block, block, jax.ShapeDtypeStruct((1, 2 * size), F32)),
        in_specs=[vmem] * 3,
        out_specs=(vmem,) * 3,
        scratch_shapes=[
            pltpu.VMEM((4, size, 2 * size), F32),
            pltpu.VMEM((width, RAW), F32),
            pltpu.VMEM((width, RAW), F32),
            pltpu.VMEM((width, 2 * size), F32),
            pltpu.VMEM((width, 2 * size), F32),
            pltpu.VMEM((width, columns - RAW), F32),
            pltpu.VMEM((NEAR, 8, 2 * size), F32),
            pltpu.VMEM((4, 8, 2 * size), F32),
            dma((3,)), dma((3,)), dma((2,)), dma((2,)), dma, dma, dma((tiles,)), dma((tiles,)),
            dma((NEAR - 1,)), dma((NEAR - 1,)), dma((3,)), dma((3,)),
        ],
        compiler_params=pltpu.CompilerParams(
            collective_id=distance, has_side_effects=True, vmem_limit_bytes=40 * 1024 * 1024
        ),
        name=f"step_{distance}",
    )(first, second, flag)


def plan_kernel(plan_ref, branch_ref, flags_ref):
    slot = jnp.int32(0)
    for index in range(STEPS):
        stays = (plan_ref[index, 1] == 1).astype(jnp.int32)
        branch_ref[index] = jnp.maximum(plan_ref[index, 0] >> 1, plan_ref[index, 1] >> 1) - 1
        leaves = ((1 - stays) == slot).astype(F32)
        flags_ref[index] = jnp.full((1, 128), leaves, F32)
        slot = stays
    flags_ref[STEPS] = jnp.full((1, 128), slot.astype(F32), F32)


def read_plan(plan):
    smem = pl.BlockSpec(memory_space=pltpu.SMEM)
    return pl.pallas_call(
        plan_kernel,
        out_shape=(
            jax.ShapeDtypeStruct((STEPS,), jnp.int32),
            jax.ShapeDtypeStruct((STEPS + 1, 1, 128), F32),
        ),
        in_specs=[smem],
        out_specs=(smem, pl.BlockSpec(memory_space=pltpu.VMEM)),
        name="read_plan",
    )(plan)


def local(columns, plan):
    cycle = lax.axis_size("blk")
    width = columns.shape[0] // 2
    branches = [partial(step, distance=distance) for distance in range(1, cycle)]
    chosen, flags = read_plan(plan)

    def one_step(index, carry):
        first, second, ratios = carry
        first, second, ratio = lax.switch(chosen[index], branches, first, second, flags[index])
        return first, second, lax.dynamic_update_slice(ratios, ratio, (index, 0))

    ratios = jnp.zeros((STEPS, 4 * width), F32)
    first, second, ratios = lax.fori_loop(0, STEPS, one_step, (columns[:width], columns[width:], ratios))
    swap = flags[STEPS, 0, :1] != 0.0
    swept = jnp.where(
        swap[:, None],
        jnp.concatenate([second, first], axis=0),
        jnp.concatenate([first, second], axis=0),
    )
    return swept, ratios[:, 0]


def solution(mesh):
    return jax.shard_map(
        local,
        mesh=mesh,
        in_specs=(P("blk", "rows"), P()),
        out_specs=(P("blk", "rows"), P()),
        check_vma=False,
    )
```

```python
from functools import partial

import jax
import jax.numpy as jnp
from jax import lax
from jax.experimental import pallas as pl
from jax.experimental.pallas import tpu as pltpu
from jax.sharding import PartitionSpec as P

STEPS = 3
EIG_ITERS = 3
NS_ITERS = 8
F32 = jnp.float32
BF16 = jnp.bfloat16
NT = (((1,), (1,)), ((), ()))
MESH = pl.DeviceIdType.MESH


def dot(left, right):
    return jnp.dot(left, right, preferred_element_type=F32)


def left_mask(shape):
    return lax.broadcasted_iota(jnp.int32, shape, 1) < shape[1] // 2


def parts(wide):
    high = wide.astype(BF16)
    rest = wide - high.astype(F32)
    middle = rest.astype(BF16)
    last = rest - middle.astype(F32)
    return high, rest, middle, last


def as_left(twice):
    high, rest, middle, last = parts(twice)
    mask = left_mask(twice.shape)
    first = jnp.where(mask, twice, rest).astype(BF16)
    second = jnp.where(mask, twice, last).astype(BF16)
    return jnp.concatenate([first, first, second], axis=1)


def as_right(wide):
    high, rest, middle, last = parts(wide)
    return jnp.concatenate([high, high, middle, middle, last.astype(BF16), high], axis=0)


def as_right_transposed(twice):
    high, rest, middle, last = parts(twice)
    mask = left_mask(twice.shape)
    third = jnp.where(mask, last, twice).astype(BF16)
    rows = jnp.concatenate([high, middle, third], axis=1)
    return jnp.concatenate([rows, rows], axis=0)


def rotation_rows(gram):
    size = gram.shape[0]
    shape = gram.shape
    row = lax.broadcasted_iota(jnp.int32, shape, 0)
    column = lax.broadcasted_iota(jnp.int32, shape, 1)
    diagonal = (column == row) | (column == row + size)
    eye = jnp.where(diagonal, 1.0, 0.0).astype(F32)
    left = left_mask(shape)
    gram_right = as_right(gram)

    def polar_turn(step, carry):
        x, total = carry
        x_right = as_right(x)
        stacked = dot(jnp.concatenate([as_left(x), as_left(total)], axis=0), x_right)
        square = stacked[:size]
        total = total + 0.5 * stacked[size:]
        return 0.75 * square + 0.25 * dot(as_left(square), x_right), total

    def turn(index, z):
        z_left = as_left(z)
        inner = lax.dot_general(z_left, as_right_transposed(z), NT, preferred_element_type=F32)
        z_gram = dot(z_left, gram_right)
        squares = jnp.where(diagonal, inner, 0.0)
        scale_row = lax.rsqrt(jnp.sum(squares, axis=0, keepdims=True))
        scale_column = lax.rsqrt(0.5 * jnp.sum(squares, axis=1, keepdims=True))
        inner = inner * scale_column * scale_row
        bound = jnp.max(jnp.sum(jnp.abs(inner), axis=0, keepdims=True), axis=1, keepdims=True)
        x = eye - inner / bound
        both = jnp.where(left, z_gram, z) * (scale_column * lax.rsqrt(bound))
        x, total = lax.fori_loop(0, NS_ITERS - 1, polar_turn, (x, eye))
        both = dot(as_left(total), as_right(both))
        both = both + 0.5 * dot(as_left(x), as_right(both))
        other = pltpu.roll(both, size, 1)
        last = index == EIG_ITERS - 1
        return jnp.where(left == jnp.logical_not(last), both, other)

    return lax.fori_loop(0, EIG_ITERS, turn, gram)


def two_parts(values):
    high = values.astype(BF16)
    return high, (values - high.astype(F32)).astype(BF16)


def left_of_three(twice):
    rest = twice - twice.astype(BF16).astype(F32)
    first = jnp.where(left_mask(twice.shape), twice, rest).astype(BF16)
    return jnp.concatenate([first, twice.astype(BF16)], axis=1)[:, : 3 * twice.shape[1] // 2]


def right_of_three(values):
    high, low = two_parts(values)
    return jnp.concatenate([high, high, low], axis=0)


RAW = 2048
NEAR = 8
TILE = 512
STATE = 8
VMEM = pl.BlockSpec(memory_space=pltpu.VMEM)
SMEM = pl.BlockSpec(memory_space=pltpu.SMEM)
ANY = pl.BlockSpec(memory_space=pl.ANY)
DMA = pltpu.SemaphoreType.DMA


def at_tile(index, start=0):
    return pl.ds(pl.multiple_of(start + index * TILE, 128), TILE)


def gram_terms(first, second):
    pieces = jnp.concatenate(two_parts(jnp.concatenate([first, second], axis=0)), axis=0)
    return lax.dot_general(pieces, pieces, NT, preferred_element_type=F32)


def step_kernel(
    distance, first_ref, second_ref, terms_ref, state_ref,
    stay_ref, come_ref, next_terms_ref, next_state_ref,
    grams, raw_first, raw_second, rows_out, rows_in, move_out, near_sums, far_sums,
    near_send, near_recv, far_send, far_recv, gram_send, gram_recv, raw_send, raw_recv, rows_send, rows_recv, move_send, move_recv,
):
    me = lax.axis_index("rows")
    count = lax.axis_size("rows")
    here = lax.axis_index("blk")
    cycle = lax.axis_size("blk")
    target = lax.rem(here + distance, cycle)
    origin = lax.rem(here + (cycle - distance), cycle)
    width, columns = first_ref.shape
    size = 2 * width
    wide = 2 * size
    tiles = (columns - RAW) // TILE

    near, far = lax.rem(here, NEAR), here // NEAR
    groups = cycle // NEAR

    def row_peer(away):
        return {"rows": lax.rem(me + away, count)}

    def near_peer(away):
        return {"blk": far * NEAR + lax.rem(near + away, NEAR)}

    def far_peer(away):
        return {"blk": lax.rem(here + away * NEAR, cycle)}

    def each(peers, body):
        def one(away, carry):
            body(away)
            return carry

        lax.fori_loop(1, peers, one, 0)

    barrier = pltpu.get_barrier_semaphore()

    def greet(device):
        pl.semaphore_signal(barrier, inc=1, device_id=device, device_id_type=MESH)

    greet({"blk": origin})
    each(count, lambda away: greet(row_peer(away)))
    each(NEAR, lambda away: greet(near_peer(away)))
    each(groups, lambda away: greet(far_peer(away)))

    def shared(buffer, slot, device, send_sem, recv_sem, away):
        return pltpu.make_async_remote_copy(
            src_ref=buffer.at[slot], dst_ref=buffer.at[slot],
            send_sem=send_sem.at[away - 1], recv_sem=recv_sem.at[away - 1],
            device_id=device, device_id_type=MESH,
        )

    def gram_copy(away):
        return shared(grams, me, row_peer(away), gram_send, gram_recv, away)

    def near_copy(away):
        return shared(near_sums, near, near_peer(away), near_send, near_recv, away)

    def far_copy(away):
        return shared(far_sums, far, far_peer(away), far_send, far_recv, away)

    def to_target(source, destination, send_sem, recv_sem):
        return pltpu.make_async_remote_copy(
            src_ref=source, dst_ref=destination, send_sem=send_sem, recv_sem=recv_sem,
            device_id={"blk": target}, device_id_type=MESH,
        )

    end = pl.ds(columns - TILE, TILE)
    terms = terms_ref[...] + gram_terms(first_ref[:, end], second_ref[:, end])
    terms = terms[:size] + terms[size:]
    part = terms + pltpu.roll(terms, size, 1)
    left = left_mask((width, wide))
    grams[me] = jnp.where(left, part[:width], part[width:])

    pl.semaphore_wait(barrier, 1 + (count - 1) + (NEAR - 1) + (groups - 1))
    each(count, lambda away: gram_copy(away).start())
    raw = [
        to_target(first_ref.at[:, pl.ds(0, RAW)], raw_first, raw_send.at[0], raw_recv.at[0]),
        to_target(second_ref.at[:, pl.ds(0, RAW)], raw_second, raw_send.at[1], raw_recv.at[1]),
    ]
    for copy in raw:
        copy.start()
    each(count, lambda away: gram_copy(away).wait())
    packed = (grams[0] + grams[1]) + (grams[2] + grams[3])
    turned = pltpu.roll(packed, size, 1)
    gram = jnp.concatenate(
        [jnp.where(left, packed, turned), jnp.where(left, turned, packed)], axis=0
    )

    row = lax.broadcasted_iota(jnp.int32, gram.shape, 0)
    column = lax.broadcasted_iota(jnp.int32, gram.shape, 1)
    squares = jnp.where(column < size, gram * gram, 0.0)
    off = jnp.sum(jnp.where(column == row, 0.0, squares), axis=0, keepdims=True)
    diag = jnp.sum(jnp.where(column == row, squares, 0.0), axis=0, keepdims=True)
    near_sums[near] = jnp.concatenate([off, diag, jnp.zeros((6, wide), F32)], axis=0)
    each(NEAR, lambda away: near_copy(away).start())
    state = state_ref[...]
    flag = state[:1]

    rotation = rotation_rows(gram)
    top, bottom = rotation[:width], rotation[width:]
    staying = flag * bottom + (1.0 - flag) * top
    leaving = flag * top + (1.0 - flag) * bottom
    rows_out[...] = leaving
    rows_copy = to_target(rows_out, rows_in, rows_send, rows_recv)
    rows_copy.start()
    weights = left_of_three(jnp.concatenate([staying, leaving], axis=0))

    def move_copy(index):
        return to_target(
            move_out.at[:, at_tile(index)], come_ref.at[:, at_tile(index, RAW)],
            move_send.at[index], move_recv.at[index],
        )

    def rotate_tile(index, carry):
        tile = at_tile(index, RAW)
        current = jnp.concatenate([first_ref[:, tile], second_ref[:, tile]], axis=0)
        rotated = dot(weights, right_of_three(current))
        stay_ref[:, tile] = rotated[:width]
        move_out[:, at_tile(index)] = rotated[width:]

        @pl.when(index == tiles - 1)
        def _():
            each(NEAR, lambda away: near_copy(away).wait())
            far_sums[far] = jnp.sum(near_sums[...], axis=0)
            each(groups, lambda away: far_copy(away).start())

        move_copy(index).start()
        return carry

    lax.fori_loop(0, tiles, rotate_tile, 0)

    for copy in raw:
        copy.wait()
    rows_copy.wait()
    arrived = left_of_three(rows_in[...])

    def come_tile(index, total):
        tile = at_tile(index)
        current = jnp.concatenate([first_ref[:, tile], second_ref[:, tile]], axis=0)
        other = jnp.concatenate([raw_first[:, tile], raw_second[:, tile]], axis=0)
        stay = dot(weights[:width], right_of_three(current))
        come = dot(arrived, right_of_three(other))
        stay_ref[:, tile] = stay
        come_ref[:, tile] = come
        return total + gram_terms(stay, come)

    total = lax.fori_loop(0, RAW // TILE, come_tile, jnp.zeros((wide, wide), F32))

    def wait_tile(index, total):
        move_copy(index).wait()
        tile = at_tile(index, RAW)
        return total + gram_terms(stay_ref[:, tile], come_ref[:, tile])

    next_terms_ref[...] = lax.fori_loop(0, tiles - 1, wait_tile, total)
    each(groups, lambda away: far_copy(away).wait())
    roots = jnp.sqrt(jnp.sum(jnp.sum(far_sums[...], axis=0)[:2], axis=1, keepdims=True))
    ratio = jnp.broadcast_to(roots[:1] / roots[1:], flag.shape)
    next_state_ref[...] = jnp.concatenate([state[1 : STEPS + 1], flag, state[STEPS + 2 :], ratio], axis=0)
    move_copy(tiles - 1).wait()


def step(first, second, terms, state, distance):
    width, columns = first.shape
    block = jax.ShapeDtypeStruct((width, columns), F32)
    size = 2 * width
    tiles = (columns - RAW) // TILE
    return pl.pallas_call(
        partial(step_kernel, distance),
        out_shape=(
            block,
            block,
            jax.ShapeDtypeStruct((2 * size, 2 * size), F32),
            jax.ShapeDtypeStruct((STATE, 2 * size), F32),
        ),
        in_specs=[VMEM] * 4,
        out_specs=(VMEM,) * 4,
        scratch_shapes=[
            pltpu.VMEM((4, width, 2 * size), F32),
            pltpu.VMEM((width, RAW), F32),
            pltpu.VMEM((width, RAW), F32),
            pltpu.VMEM((width, 2 * size), F32),
            pltpu.VMEM((width, 2 * size), F32),
            pltpu.VMEM((width, columns - RAW), F32),
            pltpu.VMEM((NEAR, 8, 2 * size), F32),
            pltpu.VMEM((4, 8, 2 * size), F32),
            DMA((NEAR - 1,)), DMA((NEAR - 1,)), DMA((3,)), DMA((3,)),
            DMA((3,)), DMA((3,)), DMA((2,)), DMA((2,)), DMA, DMA, DMA((tiles,)), DMA((tiles,)),
        ],
        compiler_params=pltpu.CompilerParams(
            collective_id=distance, has_side_effects=True, vmem_limit_bytes=40 * 1024 * 1024
        ),
        name=f"step_{distance}",
    )(first, second, terms, state)


def begin_kernel(columns_ref, plan_any, first_ref, second_ref, terms_ref, state_ref, branch_any, plan_ref, branch_ref, sems):
    width, columns = first_ref.shape
    pieces = 4
    span = columns // pieces
    plan_copy = pltpu.make_async_copy(plan_any, plan_ref, sems.at[2 * pieces])
    plan_copy.start()
    copies = []
    for index in range(pieces):
        part = pl.ds(index * span, span)
        for half, block_ref in enumerate((first_ref, second_ref)):
            copy = pltpu.make_async_copy(
                columns_ref.at[pl.ds(half * width, width), part],
                block_ref.at[:, part],
                sems.at[2 * index + half],
            )
            copy.start()
            copies.append(copy)
    plan_copy.wait()
    rows = []
    slot = jnp.int32(0)
    for index in range(STEPS):
        stays = (plan_ref[index, 1] == 1).astype(jnp.int32)
        branch_ref[index] = jnp.maximum(plan_ref[index, 0] >> 1, plan_ref[index, 1] >> 1) - 1
        rows.append(jnp.full((1, 4 * width), ((1 - stays) == slot).astype(F32), F32))
        slot = stays
    rows.append(jnp.full((1, 4 * width), slot.astype(F32), F32))
    branch_copy = pltpu.make_async_copy(branch_ref, branch_any, sems.at[2 * pieces + 1])
    branch_copy.start()
    state_ref[...] = jnp.concatenate(rows + [jnp.zeros((STATE - STEPS - 1, 4 * width), F32)], axis=0)
    total = jnp.zeros((4 * width, 4 * width), F32)
    for index in range(pieces):
        copies[2 * index].wait()
        copies[2 * index + 1].wait()
        size = span if index < pieces - 1 else span - TILE
        part = pl.ds(index * span, size)
        total = total + gram_terms(first_ref[:, part], second_ref[:, part])
    terms_ref[...] = total
    branch_copy.wait()


def begin(columns, plan):
    width = columns.shape[0] // 2
    block = jax.ShapeDtypeStruct((width, columns.shape[1]), F32)
    return pl.pallas_call(
        begin_kernel,
        out_shape=(
            block,
            block,
            jax.ShapeDtypeStruct((4 * width, 4 * width), F32),
            jax.ShapeDtypeStruct((STATE, 4 * width), F32),
            jax.ShapeDtypeStruct((STEPS,), jnp.int32),
        ),
        in_specs=[ANY, ANY],
        out_specs=(VMEM,) * 4 + (ANY,),
        scratch_shapes=[
            pltpu.SMEM(plan.shape, jnp.int32), pltpu.SMEM((STEPS,), jnp.int32), DMA((10,)),
        ],
        name="begin",
    )(columns, plan)


def finish_kernel(first_ref, second_ref, state_ref, swept_ref, ratio_ref, ratios, sems):
    width = first_ref.shape[0]
    start = pl.multiple_of(state_ref[0, 0].astype(jnp.int32) * width, width)
    copies = [
        pltpu.make_async_copy(first_ref, swept_ref.at[pl.ds(start, width)], sems.at[0]),
        pltpu.make_async_copy(second_ref, swept_ref.at[pl.ds(width - start, width)], sems.at[1]),
    ]
    for copy in copies:
        copy.start()
    for index in range(STEPS):
        ratios[index] = state_ref[STATE - STEPS + index, 0]
    copies.append(pltpu.make_async_copy(ratios, ratio_ref, sems.at[2]))
    copies[-1].start()
    for copy in copies:
        copy.wait()


def finish(first, second, state):
    width, columns = first.shape
    return pl.pallas_call(
        finish_kernel,
        out_shape=(
            jax.ShapeDtypeStruct((2 * width, columns), F32),
            jax.ShapeDtypeStruct((STEPS,), F32),
        ),
        in_specs=[VMEM, VMEM, VMEM],
        out_specs=(ANY, ANY),
        scratch_shapes=[pltpu.SMEM((STEPS,), F32), DMA((3,))],
        name="finish",
    )(first, second, state)


def local(columns, plan):
    cycle = lax.axis_size("blk")
    branches = [partial(step, distance=distance) for distance in range(1, cycle)]
    *held, chosen = begin(columns, plan)

    def one_step(index, held):
        return tuple(lax.switch(chosen[index], branches, *held))

    first, second, terms, state = lax.fori_loop(0, STEPS, one_step, tuple(held))
    return tuple(finish(first, second, state))


def solution(mesh):
    return jax.shard_map(
        local,
        mesh=mesh,
        in_specs=(P("blk", "rows"), P()),
        out_specs=(P("blk", "rows"), P()),
        check_vma=False,
    )
```

```python
from functools import partial

import jax
import jax.numpy as jnp
from jax import lax
from jax.experimental import pallas as pl
from jax.experimental.pallas import tpu as pltpu
from jax.sharding import PartitionSpec as P

STEPS = 3
EIG_ITERS = 3
NS_ITERS = 8
F32 = jnp.float32
BF16 = jnp.bfloat16
NT = (((1,), (1,)), ((), ()))
MESH = pl.DeviceIdType.MESH


def dot(left, right):
    return jnp.dot(left, right, preferred_element_type=F32)


def left_mask(shape):
    return lax.broadcasted_iota(jnp.int32, shape, 1) < shape[1] // 2


def parts(wide):
    high = wide.astype(BF16)
    rest = wide - high.astype(F32)
    middle = rest.astype(BF16)
    last = rest - middle.astype(F32)
    return high, rest, middle, last


def as_left(twice):
    high, rest, middle, last = parts(twice)
    mask = left_mask(twice.shape)
    first = jnp.where(mask, twice, rest).astype(BF16)
    second = jnp.where(mask, twice, last).astype(BF16)
    return jnp.concatenate([first, first, second], axis=1)


def as_right(wide):
    high, rest, middle, last = parts(wide)
    return jnp.concatenate([high, high, middle, middle, last.astype(BF16), high], axis=0)


def as_right_transposed(twice):
    high, rest, middle, last = parts(twice)
    mask = left_mask(twice.shape)
    third = jnp.where(mask, last, twice).astype(BF16)
    rows = jnp.concatenate([high, middle, third], axis=1)
    return jnp.concatenate([rows, rows], axis=0)


def rotation_rows(gram, between):
    size = gram.shape[0]
    shape = gram.shape
    row = lax.broadcasted_iota(jnp.int32, shape, 0)
    column = lax.broadcasted_iota(jnp.int32, shape, 1)
    diagonal = (column == row) | (column == row + size)
    eye = jnp.where(diagonal, 1.0, 0.0).astype(F32)
    left = left_mask(shape)
    gram_right = as_right(gram)

    def polar_turn(step, carry):
        x, total = carry
        x_right = as_right(x)
        stacked = dot(jnp.concatenate([as_left(x), as_left(total)], axis=0), x_right)
        square = stacked[:size]
        total = total + 0.5 * stacked[size:]
        return 0.75 * square + 0.25 * dot(as_left(square), x_right), total

    def turn(index, z):
        between(index)
        z_left = as_left(z)
        inner = lax.dot_general(z_left, as_right_transposed(z), NT, preferred_element_type=F32)
        z_gram = dot(z_left, gram_right)
        squares = jnp.where(diagonal, inner, 0.0)
        scale_row = lax.rsqrt(jnp.sum(squares, axis=0, keepdims=True))
        scale_column = lax.rsqrt(0.5 * jnp.sum(squares, axis=1, keepdims=True))
        inner = inner * scale_column * scale_row
        bound = jnp.max(jnp.sum(jnp.abs(inner), axis=0, keepdims=True), axis=1, keepdims=True)
        x = eye - inner / bound
        both = jnp.where(left, z_gram, z) * (scale_column * lax.rsqrt(bound))
        x, total = lax.fori_loop(0, NS_ITERS - 1, polar_turn, (x, eye))
        both = dot(as_left(total), as_right(both))
        both = both + 0.5 * dot(as_left(x), as_right(both))
        other = pltpu.roll(both, size, 1)
        last = index == EIG_ITERS - 1
        return jnp.where(left == jnp.logical_not(last), both, other)

    return lax.fori_loop(0, EIG_ITERS, turn, gram)


def two_parts(values):
    high = values.astype(BF16)
    return high, (values - high.astype(F32)).astype(BF16)


def left_of_three(twice):
    rest = twice - twice.astype(BF16).astype(F32)
    first = jnp.where(left_mask(twice.shape), twice, rest).astype(BF16)
    return jnp.concatenate([first, twice.astype(BF16)], axis=1)[:, : 3 * twice.shape[1] // 2]


def right_of_three(values):
    high, low = two_parts(values)
    return jnp.concatenate([high, high, low], axis=0)


RAW = 2048
NEAR = 8
CORES = 2
TILE = 512
STATE = 16
VMEM = pl.BlockSpec(memory_space=pltpu.VMEM)
SMEM = pl.BlockSpec(memory_space=pltpu.SMEM)
ANY = pl.BlockSpec(memory_space=pl.ANY)
DMA = pltpu.SemaphoreType.DMA


def at_tile(index, start=0):
    return pl.ds(pl.multiple_of(start + index * TILE, 128), TILE)


def gram_terms(first, second):
    pieces = jnp.concatenate(two_parts(jnp.concatenate([first, second], axis=0)), axis=0)
    return lax.dot_general(pieces, pieces, NT, preferred_element_type=F32)


def step_kernel(
    distance, first_ref, second_ref, terms_ref, state_ref,
    stay_ref, come_ref, next_terms_ref, next_state_ref,
    grams, raw_first, raw_second, rows_out, rows_in, move_out, core_sums, near_sums, far_sums,
    core_send, core_recv,
    near_send, near_recv, far_send, far_recv, gram_send, gram_recv, raw_send, raw_recv, rows_send, rows_recv, move_send, move_recv,
):
    me = lax.axis_index("rows")
    count = lax.axis_size("rows")
    here = lax.axis_index("blk")
    cycle = lax.axis_size("blk")
    target = lax.rem(here + distance, cycle)
    origin = lax.rem(here + (cycle - distance), cycle)
    width, columns = first_ref.shape
    size = 2 * width
    wide = 2 * size
    tiles = (columns - RAW) // TILE

    core, near, far = lax.rem(here, CORES), lax.rem(here, NEAR) // CORES, here // NEAR
    line, groups = NEAR // CORES, cycle // NEAR

    def row_peer(away):
        return {"rows": lax.rem(me + away, count)}

    def near_peer(away):
        return {"blk": far * NEAR + lax.rem(near + away, line) * CORES + core}

    def core_peer(away):
        return {"blk": here + away - 2 * core}

    def far_peer(away):
        return {"blk": lax.rem(here + away * NEAR, cycle)}

    def each(peers, body):
        def one(away, carry):
            body(away)
            return carry

        lax.fori_loop(1, peers, one, 0)

    barrier = pltpu.get_barrier_semaphore()

    def greet(device):
        pl.semaphore_signal(barrier, inc=1, device_id=device, device_id_type=MESH)

    greet({"blk": origin})
    each(count, lambda away: greet(row_peer(away)))
    greet(core_peer(1))
    each(line, lambda away: greet(near_peer(away)))
    each(groups, lambda away: greet(far_peer(away)))

    def shared(buffer, slot, device, send_sem, recv_sem, away):
        return pltpu.make_async_remote_copy(
            src_ref=buffer.at[slot], dst_ref=buffer.at[slot],
            send_sem=send_sem.at[away - 1], recv_sem=recv_sem.at[away - 1],
            device_id=device, device_id_type=MESH,
        )

    def gram_copy(away):
        return shared(grams, me, row_peer(away), gram_send, gram_recv, away)

    def core_copy(away):
        return shared(core_sums, core, core_peer(away), core_send, core_recv, away)

    def near_copy(away):
        return shared(near_sums, near, near_peer(away), near_send, near_recv, away)

    def far_copy(away):
        return shared(far_sums, far, far_peer(away), far_send, far_recv, away)

    def to_target(source, destination, send_sem, recv_sem):
        return pltpu.make_async_remote_copy(
            src_ref=source, dst_ref=destination, send_sem=send_sem, recv_sem=recv_sem,
            device_id={"blk": target}, device_id_type=MESH,
        )

    end = pl.ds(columns - TILE, TILE)
    terms = terms_ref[...] + gram_terms(first_ref[:, end], second_ref[:, end])
    terms = terms[:size] + terms[size:]
    part = terms + pltpu.roll(terms, size, 1)
    left = left_mask((width, wide))
    grams[me] = jnp.where(left, part[:width], part[width:])

    pl.semaphore_wait(barrier, 1 + (count - 1) + (CORES - 1) + (line - 1) + (groups - 1))
    each(count, lambda away: gram_copy(away).start())
    raw = [
        to_target(first_ref.at[:, pl.ds(0, RAW)], raw_first, raw_send.at[0], raw_recv.at[0]),
        to_target(second_ref.at[:, pl.ds(0, RAW)], raw_second, raw_send.at[1], raw_recv.at[1]),
    ]
    for copy in raw:
        copy.start()
    each(count, lambda away: gram_copy(away).wait())
    packed = (grams[0] + grams[1]) + (grams[2] + grams[3])
    turned = pltpu.roll(packed, size, 1)
    gram = jnp.concatenate(
        [jnp.where(left, packed, turned), jnp.where(left, turned, packed)], axis=0
    )

    row = lax.broadcasted_iota(jnp.int32, gram.shape, 0)
    column = lax.broadcasted_iota(jnp.int32, gram.shape, 1)
    squares = jnp.where(column < size, gram * gram, 0.0)
    off = jnp.sum(jnp.where(column == row, 0.0, squares), axis=0, keepdims=True)
    diag = jnp.sum(jnp.where(column == row, squares, 0.0), axis=0, keepdims=True)
    core_sums[core] = jnp.concatenate([off, diag, jnp.zeros((6, wide), F32)], axis=0)
    core_copy(1).start()
    state = state_ref[...]
    flag = state[:1]

    def between(index):
        @pl.when(index == 1)
        def _():
            core_copy(1).wait()
            near_sums[near] = core_sums[0] + core_sums[1]
            each(line, lambda away: near_copy(away).start())

    rotation = rotation_rows(gram, between)
    top, bottom = rotation[:width], rotation[width:]
    staying = flag * bottom + (1.0 - flag) * top
    leaving = flag * top + (1.0 - flag) * bottom
    rows_out[...] = leaving
    rows_copy = to_target(rows_out, rows_in, rows_send, rows_recv)
    rows_copy.start()
    weights = left_of_three(jnp.concatenate([staying, leaving], axis=0))

    def move_copy(index):
        return to_target(
            move_out.at[:, at_tile(index)], come_ref.at[:, at_tile(index, RAW)],
            move_send.at[index], move_recv.at[index],
        )

    def rotate_tile(index, carry):
        tile = at_tile(index, RAW)
        current = jnp.concatenate([first_ref[:, tile], second_ref[:, tile]], axis=0)
        rotated = dot(weights, right_of_three(current))
        stay_ref[:, tile] = rotated[:width]
        move_out[:, at_tile(index)] = rotated[width:]

        @pl.when(index == tiles - 1)
        def _():
            each(line, lambda away: near_copy(away).wait())
            far_sums[far] = jnp.sum(near_sums[...], axis=0)
            each(groups, lambda away: far_copy(away).start())

        move_copy(index).start()
        return carry

    lax.fori_loop(0, tiles, rotate_tile, 0)

    for copy in raw:
        copy.wait()
    rows_copy.wait()
    arrived = left_of_three(rows_in[...])

    def come_tile(index, total):
        tile = at_tile(index)
        current = jnp.concatenate([first_ref[:, tile], second_ref[:, tile]], axis=0)
        other = jnp.concatenate([raw_first[:, tile], raw_second[:, tile]], axis=0)
        stay = dot(weights[:width], right_of_three(current))
        come = dot(arrived, right_of_three(other))
        stay_ref[:, tile] = stay
        come_ref[:, tile] = come
        return total + gram_terms(stay, come)

    total = lax.fori_loop(0, RAW // TILE, come_tile, jnp.zeros((wide, wide), F32))

    def wait_tile(index, total):
        move_copy(index).wait()
        tile = at_tile(index, RAW)
        return total + gram_terms(stay_ref[:, tile], come_ref[:, tile])

    next_terms_ref[...] = lax.fori_loop(0, tiles - 1, wait_tile, total)
    each(groups, lambda away: far_copy(away).wait())
    totals = jnp.sum(far_sums[...], axis=0)
    next_state_ref[...] = jnp.concatenate(
        [state[1 : STEPS + 1], flag, state[STEPS + 1 : 8], state[10:], totals[:2]], axis=0
    )
    move_copy(tiles - 1).wait()


def step(first, second, terms, state, distance):
    width, columns = first.shape
    block = jax.ShapeDtypeStruct((width, columns), F32)
    size = 2 * width
    tiles = (columns - RAW) // TILE
    return pl.pallas_call(
        partial(step_kernel, distance),
        out_shape=(
            block,
            block,
            jax.ShapeDtypeStruct((2 * size, 2 * size), F32),
            jax.ShapeDtypeStruct((STATE, 2 * size), F32),
        ),
        in_specs=[VMEM] * 4,
        out_specs=(VMEM,) * 4,
        scratch_shapes=[
            pltpu.VMEM((4, width, 2 * size), F32),
            pltpu.VMEM((width, RAW), F32),
            pltpu.VMEM((width, RAW), F32),
            pltpu.VMEM((width, 2 * size), F32),
            pltpu.VMEM((width, 2 * size), F32),
            pltpu.VMEM((width, columns - RAW), F32),
            pltpu.VMEM((CORES, 8, 2 * size), F32),
            pltpu.VMEM((NEAR // CORES, 8, 2 * size), F32),
            pltpu.VMEM((4, 8, 2 * size), F32),
            DMA((1,)), DMA((1,)), DMA((3,)), DMA((3,)), DMA((3,)), DMA((3,)),
            DMA((3,)), DMA((3,)), DMA((2,)), DMA((2,)), DMA, DMA, DMA((tiles,)), DMA((tiles,)),
        ],
        compiler_params=pltpu.CompilerParams(
            collective_id=distance, has_side_effects=True, vmem_limit_bytes=40 * 1024 * 1024
        ),
        name=f"step_{distance}",
    )(first, second, terms, state)


def begin_kernel(columns_ref, plan_any, first_ref, second_ref, terms_ref, state_ref, branch_any, plan_ref, branch_ref, sems):
    width, columns = first_ref.shape
    pieces = 4
    span = columns // pieces
    plan_copy = pltpu.make_async_copy(plan_any, plan_ref, sems.at[2 * pieces])
    plan_copy.start()
    copies = []
    for index in range(pieces):
        part = pl.ds(index * span, span)
        for half, block_ref in enumerate((first_ref, second_ref)):
            copy = pltpu.make_async_copy(
                columns_ref.at[pl.ds(half * width, width), part],
                block_ref.at[:, part],
                sems.at[2 * index + half],
            )
            copy.start()
            copies.append(copy)
    plan_copy.wait()
    rows = []
    slot = jnp.int32(0)
    for index in range(STEPS):
        stays = (plan_ref[index, 1] == 1).astype(jnp.int32)
        branch_ref[index] = jnp.maximum(plan_ref[index, 0] >> 1, plan_ref[index, 1] >> 1) - 1
        rows.append(jnp.full((1, 4 * width), ((1 - stays) == slot).astype(F32), F32))
        slot = stays
    rows.append(jnp.full((1, 4 * width), slot.astype(F32), F32))
    branch_copy = pltpu.make_async_copy(branch_ref, branch_any, sems.at[2 * pieces + 1])
    branch_copy.start()
    state_ref[...] = jnp.concatenate(rows + [jnp.zeros((STATE - STEPS - 1, 4 * width), F32)], axis=0)
    total = jnp.zeros((4 * width, 4 * width), F32)
    for index in range(pieces):
        copies[2 * index].wait()
        copies[2 * index + 1].wait()
        size = span if index < pieces - 1 else span - TILE
        part = pl.ds(index * span, size)
        total = total + gram_terms(first_ref[:, part], second_ref[:, part])
    terms_ref[...] = total
    branch_copy.wait()


def begin(columns, plan):
    width = columns.shape[0] // 2
    block = jax.ShapeDtypeStruct((width, columns.shape[1]), F32)
    return pl.pallas_call(
        begin_kernel,
        out_shape=(
            block,
            block,
            jax.ShapeDtypeStruct((4 * width, 4 * width), F32),
            jax.ShapeDtypeStruct((STATE, 4 * width), F32),
            jax.ShapeDtypeStruct((STEPS,), jnp.int32),
        ),
        in_specs=[ANY, ANY],
        out_specs=(VMEM,) * 4 + (ANY,),
        scratch_shapes=[
            pltpu.SMEM(plan.shape, jnp.int32), pltpu.SMEM((STEPS,), jnp.int32), DMA((10,)),
        ],
        name="begin",
    )(columns, plan)


def finish_kernel(first_ref, second_ref, state_ref, swept_ref, ratio_ref, ratios, sems):
    width = first_ref.shape[0]
    start = pl.multiple_of(state_ref[0, 0].astype(jnp.int32) * width, width)
    copies = [
        pltpu.make_async_copy(first_ref, swept_ref.at[pl.ds(start, width)], sems.at[0]),
        pltpu.make_async_copy(second_ref, swept_ref.at[pl.ds(width - start, width)], sems.at[1]),
    ]
    for copy in copies:
        copy.start()
    roots = jnp.sqrt(jnp.sum(state_ref[STATE - 8 :], axis=1, keepdims=True))
    for index in range(STEPS):
        row = 8 - 2 * (STEPS - index)
        ratios[index] = (roots[row : row + 1] / roots[row + 1 : row + 2])[0, 0]
    copies.append(pltpu.make_async_copy(ratios, ratio_ref, sems.at[2]))
    copies[-1].start()
    for copy in copies:
        copy.wait()


def finish(first, second, state):
    width, columns = first.shape
    return pl.pallas_call(
        finish_kernel,
        out_shape=(
            jax.ShapeDtypeStruct((2 * width, columns), F32),
            jax.ShapeDtypeStruct((STEPS,), F32),
        ),
        in_specs=[VMEM, VMEM, VMEM],
        out_specs=(ANY, ANY),
        scratch_shapes=[pltpu.SMEM((STEPS,), F32), DMA((3,))],
        name="finish",
    )(first, second, state)


def local(columns, plan):
    cycle = lax.axis_size("blk")
    branches = [partial(step, distance=distance) for distance in range(1, cycle)]
    *held, chosen = begin(columns, plan)

    def one_step(index, held):
        return tuple(lax.switch(chosen[index], branches, *held))

    first, second, terms, state = lax.fori_loop(0, STEPS, one_step, tuple(held))
    return tuple(finish(first, second, state))


def solution(mesh):
    return jax.shard_map(
        local,
        mesh=mesh,
        in_specs=(P("blk", "rows"), P()),
        out_specs=(P("blk", "rows"), P()),
        check_vma=False,
    )
```

```python
from functools import partial

import jax
import jax.numpy as jnp
from jax import lax
from jax.experimental import pallas as pl
from jax.experimental.pallas import tpu as pltpu
from jax.sharding import PartitionSpec as P

STEPS = 3
EIG_ITERS = 3
NS_ITERS = 8
F32 = jnp.float32
BF16 = jnp.bfloat16
NT = (((1,), (1,)), ((), ()))
MESH = pl.DeviceIdType.MESH


def dot(left, right):
    return jnp.dot(left, right, preferred_element_type=F32)


def left_mask(shape):
    return lax.broadcasted_iota(jnp.int32, shape, 1) < shape[1] // 2


def parts(wide):
    high = wide.astype(BF16)
    rest = wide - high.astype(F32)
    middle = rest.astype(BF16)
    last = rest - middle.astype(F32)
    return high, rest, middle, last


def as_left(twice):
    high, rest, middle, last = parts(twice)
    mask = left_mask(twice.shape)
    first = jnp.where(mask, twice, rest).astype(BF16)
    second = jnp.where(mask, twice, last).astype(BF16)
    return jnp.concatenate([first, first, second], axis=1)


def as_right(wide):
    high, rest, middle, last = parts(wide)
    return jnp.concatenate([high, high, middle, middle, last.astype(BF16), high], axis=0)


def as_right_transposed(twice):
    high, rest, middle, last = parts(twice)
    mask = left_mask(twice.shape)
    third = jnp.where(mask, last, twice).astype(BF16)
    rows = jnp.concatenate([high, middle, third], axis=1)
    return jnp.concatenate([rows, rows], axis=0)


def rotation_rows(gram, between):
    size = gram.shape[0]
    shape = gram.shape
    row = lax.broadcasted_iota(jnp.int32, shape, 0)
    column = lax.broadcasted_iota(jnp.int32, shape, 1)
    diagonal = (column == row) | (column == row + size)
    eye = jnp.where(diagonal, 1.0, 0.0).astype(F32)
    left = left_mask(shape)
    gram_right = as_right(gram)

    def polar_turn(step, carry):
        x, total = carry
        x_right = as_right(x)
        stacked = dot(jnp.concatenate([as_left(x), as_left(total)], axis=0), x_right)
        square = stacked[:size]
        total = total + 0.5 * stacked[size:]
        return 0.75 * square + 0.25 * dot(as_left(square), x_right), total

    def turn(index, z):
        between(index)
        z_left = as_left(z)
        inner = lax.dot_general(z_left, as_right_transposed(z), NT, preferred_element_type=F32)
        z_gram = dot(z_left, gram_right)
        squares = jnp.where(diagonal, inner, 0.0)
        scale_row = lax.rsqrt(jnp.sum(squares, axis=0, keepdims=True))
        scale_column = lax.rsqrt(0.5 * jnp.sum(squares, axis=1, keepdims=True))
        inner = inner * scale_column * scale_row
        bound = jnp.max(jnp.sum(jnp.abs(inner), axis=0, keepdims=True), axis=1, keepdims=True)
        x = eye - inner / bound
        both = jnp.where(left, z_gram, z) * (scale_column * lax.rsqrt(bound))
        x, total = lax.fori_loop(0, NS_ITERS - 1, polar_turn, (x, eye))
        both = dot(as_left(total), as_right(both))
        both = both + 0.5 * dot(as_left(x), as_right(both))
        other = pltpu.roll(both, size, 1)
        last = index == EIG_ITERS - 1
        return jnp.where(left == jnp.logical_not(last), both, other)

    return lax.fori_loop(0, EIG_ITERS, turn, gram)


def two_parts(values):
    high = values.astype(BF16)
    return high, (values - high.astype(F32)).astype(BF16)


def left_of_three(twice):
    rest = twice - twice.astype(BF16).astype(F32)
    first = jnp.where(left_mask(twice.shape), twice, rest).astype(BF16)
    return jnp.concatenate([first, twice.astype(BF16)], axis=1)[:, : 3 * twice.shape[1] // 2]


def right_of_three(values):
    high, low = two_parts(values)
    return jnp.concatenate([high, high, low], axis=0)


RAW = 2048
NEAR = 8
CORES = 2
TILE = 512
STATE = 16
VMEM = pl.BlockSpec(memory_space=pltpu.VMEM)
SMEM = pl.BlockSpec(memory_space=pltpu.SMEM)
ANY = pl.BlockSpec(memory_space=pl.ANY)
DMA = pltpu.SemaphoreType.DMA


def at_tile(index, start=0):
    return pl.ds(pl.multiple_of(start + index * TILE, 128), TILE)


def gram_terms(first, second):
    pieces = jnp.concatenate(two_parts(jnp.concatenate([first, second], axis=0)), axis=0)
    return lax.dot_general(pieces, pieces, NT, preferred_element_type=F32)


def step_kernel(
    distance, first_ref, second_ref, terms_ref, state_ref,
    stay_ref, come_ref, next_terms_ref, next_state_ref,
    grams, raw_first, raw_second, rows_out, rows_in, move_out, core_sums, near_sums, far_sums,
    core_send, core_recv,
    near_send, near_recv, far_send, far_recv, gram_send, gram_recv, raw_send, raw_recv, rows_send, rows_recv, move_send, move_recv,
):
    me = lax.axis_index("rows")
    count = lax.axis_size("rows")
    here = lax.axis_index("blk")
    cycle = lax.axis_size("blk")
    target = lax.rem(here + distance, cycle)
    origin = lax.rem(here + (cycle - distance), cycle)
    width, columns = first_ref.shape
    size = 2 * width
    wide = 2 * size
    tiles = (columns - RAW) // TILE

    core, near, far = lax.rem(here, CORES), lax.rem(here, NEAR) // CORES, here // NEAR
    line, groups = NEAR // CORES, cycle // NEAR

    def row_peer(away):
        return {"rows": lax.rem(me + away, count)}

    def near_peer(away):
        return {"blk": far * NEAR + lax.rem(near + away, line) * CORES + core}

    def core_peer(away):
        return {"blk": here + away - 2 * core}

    def far_peer(away):
        return {"blk": lax.rem(here + away * NEAR, cycle)}

    def each(peers, body):
        def one(away, carry):
            body(away)
            return carry

        lax.fori_loop(1, peers, one, 0)

    barrier = pltpu.get_barrier_semaphore()

    def greet(device):
        pl.semaphore_signal(barrier, inc=1, device_id=device, device_id_type=MESH)

    greet({"blk": origin})
    each(count, lambda away: greet(row_peer(away)))
    greet(core_peer(1))
    each(line, lambda away: greet(near_peer(away)))
    each(groups, lambda away: greet(far_peer(away)))

    def shared(buffer, slot, device, send_sem, recv_sem, away):
        return pltpu.make_async_remote_copy(
            src_ref=buffer.at[slot], dst_ref=buffer.at[slot],
            send_sem=send_sem.at[away - 1], recv_sem=recv_sem.at[away - 1],
            device_id=device, device_id_type=MESH,
        )

    def gram_copy(away):
        return shared(grams, me, row_peer(away), gram_send, gram_recv, away)

    def core_copy(away):
        return shared(core_sums, core, core_peer(away), core_send, core_recv, away)

    def near_copy(away):
        return shared(near_sums, near, near_peer(away), near_send, near_recv, away)

    def far_copy(away):
        return shared(far_sums, far, far_peer(away), far_send, far_recv, away)

    def to_target(source, destination, send_sem, recv_sem):
        return pltpu.make_async_remote_copy(
            src_ref=source, dst_ref=destination, send_sem=send_sem, recv_sem=recv_sem,
            device_id={"blk": target}, device_id_type=MESH,
        )

    end = pl.ds(columns - TILE, TILE)
    terms = terms_ref[...] + gram_terms(first_ref[:, end], second_ref[:, end])
    terms = terms[:size] + terms[size:]
    part = terms + pltpu.roll(terms, size, 1)
    left = left_mask((width, wide))
    grams[me] = jnp.where(left, part[:width], part[width:])

    pl.semaphore_wait(barrier, 1 + (count - 1) + (CORES - 1) + (line - 1) + (groups - 1))
    each(count, lambda away: gram_copy(away).start())
    raw = [
        to_target(first_ref.at[:, pl.ds(0, RAW)], raw_first, raw_send.at[0], raw_recv.at[0]),
        to_target(second_ref.at[:, pl.ds(0, RAW)], raw_second, raw_send.at[1], raw_recv.at[1]),
    ]
    for copy in raw:
        copy.start()
    each(count, lambda away: gram_copy(away).wait())
    packed = (grams[0] + grams[1]) + (grams[2] + grams[3])
    turned = pltpu.roll(packed, size, 1)
    gram = jnp.concatenate(
        [jnp.where(left, packed, turned), jnp.where(left, turned, packed)], axis=0
    )

    row = lax.broadcasted_iota(jnp.int32, gram.shape, 0)
    column = lax.broadcasted_iota(jnp.int32, gram.shape, 1)
    squares = jnp.where(column < size, gram * gram, 0.0)
    off = jnp.sum(jnp.where(column == row, 0.0, squares), axis=0, keepdims=True)
    diag = jnp.sum(jnp.where(column == row, squares, 0.0), axis=0, keepdims=True)
    core_sums[core] = jnp.concatenate([off, diag, jnp.zeros((6, wide), F32)], axis=0)
    core_copy(1).start()
    state = state_ref[...]
    flag = state[:1]

    def between(index):
        @pl.when(index == 1)
        def _():
            core_copy(1).wait()
            near_sums[near] = core_sums[0] + core_sums[1]
            each(line, lambda away: near_copy(away).start())

    rotation = rotation_rows(gram, between)
    top, bottom = rotation[:width], rotation[width:]
    staying = flag * bottom + (1.0 - flag) * top
    leaving = flag * top + (1.0 - flag) * bottom
    rows_out[...] = leaving
    rows_copy = to_target(rows_out, rows_in, rows_send, rows_recv)
    rows_copy.start()
    weights = left_of_three(jnp.concatenate([staying, leaving], axis=0))

    def move_copy(index):
        return to_target(
            move_out.at[:, at_tile(index)], come_ref.at[:, at_tile(index, RAW)],
            move_send.at[index], move_recv.at[index],
        )

    def rotate_tile(index, carry):
        tile = at_tile(index, RAW)
        current = jnp.concatenate([first_ref[:, tile], second_ref[:, tile]], axis=0)
        rotated = dot(weights, right_of_three(current))
        stay_ref[:, tile] = rotated[:width]
        move_out[:, at_tile(index)] = rotated[width:]

        @pl.when(index == tiles - 1)
        def _():
            each(line, lambda away: near_copy(away).wait())
            far_sums[far] = jnp.sum(near_sums[...], axis=0)
            each(groups, lambda away: far_copy(away).start())

        move_copy(index).start()
        return carry

    lax.fori_loop(0, tiles, rotate_tile, 0)

    for copy in raw:
        copy.wait()
    rows_copy.wait()
    arrived = left_of_three(rows_in[...])

    def come_tile(index, total):
        tile = at_tile(index)
        current = jnp.concatenate([first_ref[:, tile], second_ref[:, tile]], axis=0)
        other = jnp.concatenate([raw_first[:, tile], raw_second[:, tile]], axis=0)
        stay = dot(weights[:width], right_of_three(current))
        come = dot(arrived, right_of_three(other))
        stay_ref[:, tile] = stay
        come_ref[:, tile] = come
        return total + gram_terms(stay, come)

    total = lax.fori_loop(0, RAW // TILE, come_tile, jnp.zeros((wide, wide), F32))

    def wait_tile(index, total):
        move_copy(index).wait()
        tile = at_tile(index, RAW)
        return total + gram_terms(stay_ref[:, tile], come_ref[:, tile])

    next_terms_ref[...] = lax.fori_loop(0, tiles - 1, wait_tile, total)
    each(groups, lambda away: far_copy(away).wait())
    totals = jnp.sum(far_sums[...], axis=0)
    next_state_ref[...] = jnp.concatenate(
        [state[1 : STEPS + 1], flag, state[STEPS + 1 : 8], state[10:], totals[:2]], axis=0
    )
    move_copy(tiles - 1).wait()


def step(first, second, terms, state, distance):
    width, columns = first.shape
    block = jax.ShapeDtypeStruct((width, columns), F32)
    size = 2 * width
    tiles = (columns - RAW) // TILE
    return pl.pallas_call(
        partial(step_kernel, distance),
        out_shape=(
            block,
            block,
            jax.ShapeDtypeStruct((2 * size, 2 * size), F32),
            jax.ShapeDtypeStruct((STATE, 2 * size), F32),
        ),
        in_specs=[VMEM] * 4,
        out_specs=(VMEM,) * 4,
        scratch_shapes=[
            pltpu.VMEM((4, width, 2 * size), F32),
            pltpu.VMEM((width, RAW), F32),
            pltpu.VMEM((width, RAW), F32),
            pltpu.VMEM((width, 2 * size), F32),
            pltpu.VMEM((width, 2 * size), F32),
            pltpu.VMEM((width, columns - RAW), F32),
            pltpu.VMEM((CORES, 8, 2 * size), F32),
            pltpu.VMEM((NEAR // CORES, 8, 2 * size), F32),
            pltpu.VMEM((4, 8, 2 * size), F32),
            DMA((1,)), DMA((1,)), DMA((3,)), DMA((3,)), DMA((3,)), DMA((3,)),
            DMA((3,)), DMA((3,)), DMA((2,)), DMA((2,)), DMA, DMA, DMA((tiles,)), DMA((tiles,)),
        ],
        compiler_params=pltpu.CompilerParams(
            collective_id=distance, has_side_effects=True, vmem_limit_bytes=40 * 1024 * 1024
        ),
        name=f"step_{distance}",
    )(first, second, terms, state)


def begin_kernel(columns_ref, plan_any, first_ref, second_ref, terms_ref, state_ref, branch_any, plan_ref, branch_ref, sems):
    width, columns = first_ref.shape
    pieces = 2
    span = columns // pieces
    plan_copy = pltpu.make_async_copy(plan_any, plan_ref, sems.at[2 * pieces])
    plan_copy.start()
    copies = []
    for index in range(pieces):
        part = pl.ds(index * span, span)
        for half, block_ref in enumerate((first_ref, second_ref)):
            copy = pltpu.make_async_copy(
                columns_ref.at[pl.ds(half * width, width), part],
                block_ref.at[:, part],
                sems.at[2 * index + half],
            )
            copy.start()
            copies.append(copy)
    plan_copy.wait()
    rows = []
    slot = jnp.int32(0)
    for index in range(STEPS):
        stays = (plan_ref[index, 1] == 1).astype(jnp.int32)
        branch_ref[index] = jnp.maximum(plan_ref[index, 0] >> 1, plan_ref[index, 1] >> 1) - 1
        rows.append(jnp.full((1, 4 * width), ((1 - stays) == slot).astype(F32), F32))
        slot = stays
    rows.append(jnp.full((1, 4 * width), slot.astype(F32), F32))
    branch_copy = pltpu.make_async_copy(branch_ref, branch_any, sems.at[2 * pieces + 1])
    branch_copy.start()
    state_ref[...] = jnp.concatenate(rows + [jnp.zeros((STATE - STEPS - 1, 4 * width), F32)], axis=0)
    total = jnp.zeros((4 * width, 4 * width), F32)
    for index in range(pieces):
        copies[2 * index].wait()
        copies[2 * index + 1].wait()
        size = span if index < pieces - 1 else span - TILE
        part = pl.ds(index * span, size)
        total = total + gram_terms(first_ref[:, part], second_ref[:, part])
    terms_ref[...] = total
    branch_copy.wait()


def begin(columns, plan):
    width = columns.shape[0] // 2
    block = jax.ShapeDtypeStruct((width, columns.shape[1]), F32)
    return pl.pallas_call(
        begin_kernel,
        out_shape=(
            block,
            block,
            jax.ShapeDtypeStruct((4 * width, 4 * width), F32),
            jax.ShapeDtypeStruct((STATE, 4 * width), F32),
            jax.ShapeDtypeStruct((STEPS,), jnp.int32),
        ),
        in_specs=[ANY, ANY],
        out_specs=(VMEM,) * 4 + (ANY,),
        scratch_shapes=[
            pltpu.SMEM(plan.shape, jnp.int32), pltpu.SMEM((STEPS,), jnp.int32), DMA((10,)),
        ],
        name="begin",
    )(columns, plan)


def finish_kernel(first_ref, second_ref, state_ref, swept_ref, ratio_ref, ratios, sems):
    width = first_ref.shape[0]
    start = pl.multiple_of(state_ref[0, 0].astype(jnp.int32) * width, width)
    copies = [
        pltpu.make_async_copy(first_ref, swept_ref.at[pl.ds(start, width)], sems.at[0]),
        pltpu.make_async_copy(second_ref, swept_ref.at[pl.ds(width - start, width)], sems.at[1]),
    ]
    for copy in copies:
        copy.start()
    roots = jnp.sqrt(jnp.sum(state_ref[STATE - 8 :], axis=1, keepdims=True))
    for index in range(STEPS):
        row = 8 - 2 * (STEPS - index)
        ratios[index] = (roots[row : row + 1] / roots[row + 1 : row + 2])[0, 0]
    copies.append(pltpu.make_async_copy(ratios, ratio_ref, sems.at[2]))
    copies[-1].start()
    for copy in copies:
        copy.wait()


def finish(first, second, state):
    width, columns = first.shape
    return pl.pallas_call(
        finish_kernel,
        out_shape=(
            jax.ShapeDtypeStruct((2 * width, columns), F32),
            jax.ShapeDtypeStruct((STEPS,), F32),
        ),
        in_specs=[VMEM, VMEM, VMEM],
        out_specs=(ANY, ANY),
        scratch_shapes=[pltpu.SMEM((STEPS,), F32), DMA((3,))],
        name="finish",
    )(first, second, state)


def local(columns, plan):
    cycle = lax.axis_size("blk")
    branches = [partial(step, distance=distance) for distance in range(1, cycle)]
    *held, chosen = begin(columns, plan)

    def one_step(index, held):
        return tuple(lax.switch(chosen[index], branches, *held))

    first, second, terms, state = lax.fori_loop(0, STEPS, one_step, tuple(held))
    return tuple(finish(first, second, state))


def solution(mesh):
    return jax.shard_map(
        local,
        mesh=mesh,
        in_specs=(P("blk", "rows"), P()),
        out_specs=(P("blk", "rows"), P()),
        check_vma=False,
    )
```

```python
from functools import partial

import jax
import jax.numpy as jnp
from jax import lax
from jax.experimental import pallas as pl
from jax.experimental.pallas import tpu as pltpu
from jax.sharding import PartitionSpec as P

STEPS = 3
EIG_ITERS = 3
NS_ITERS = 8
F32 = jnp.float32
BF16 = jnp.bfloat16
NT = (((1,), (1,)), ((), ()))
MESH = pl.DeviceIdType.MESH


def dot(left, right):
    return jnp.dot(left, right, preferred_element_type=F32)


def left_mask(shape):
    return lax.broadcasted_iota(jnp.int32, shape, 1) < shape[1] // 2


def parts(wide):
    high = wide.astype(BF16)
    rest = wide - high.astype(F32)
    middle = rest.astype(BF16)
    last = rest - middle.astype(F32)
    return high, rest, middle, last


def as_left(twice):
    high, rest, middle, last = parts(twice)
    mask = left_mask(twice.shape)
    first = jnp.where(mask, twice, rest).astype(BF16)
    second = jnp.where(mask, twice, last).astype(BF16)
    return jnp.concatenate([first, first, second], axis=1)


def as_right(wide):
    high, rest, middle, last = parts(wide)
    return jnp.concatenate([high, high, middle, middle, last.astype(BF16), high], axis=0)


def as_right_transposed(twice):
    high, rest, middle, last = parts(twice)
    mask = left_mask(twice.shape)
    third = jnp.where(mask, last, twice).astype(BF16)
    rows = jnp.concatenate([high, middle, third], axis=1)
    return jnp.concatenate([rows, rows], axis=0)


def rotation_rows(gram, between):
    size = gram.shape[0]
    shape = gram.shape
    row = lax.broadcasted_iota(jnp.int32, shape, 0)
    column = lax.broadcasted_iota(jnp.int32, shape, 1)
    diagonal = (column == row) | (column == row + size)
    eye = jnp.where(diagonal, 1.0, 0.0).astype(F32)
    left = left_mask(shape)
    gram_right = as_right(gram)

    def polar_turn(step, carry):
        x, total = carry
        x_right = as_right(x)
        stacked = dot(jnp.concatenate([as_left(x), as_left(total)], axis=0), x_right)
        square = stacked[:size]
        total = total + 0.5 * stacked[size:]
        return 0.75 * square + 0.25 * dot(as_left(square), x_right), total

    def turn(index, z):
        between(index)
        z_left = as_left(z)
        inner = lax.dot_general(z_left, as_right_transposed(z), NT, preferred_element_type=F32)
        z_gram = dot(z_left, gram_right)
        squares = jnp.where(diagonal, inner, 0.0)
        scale_row = lax.rsqrt(jnp.sum(squares, axis=0, keepdims=True))
        scale_column = lax.rsqrt(0.5 * jnp.sum(squares, axis=1, keepdims=True))
        inner = inner * scale_column * scale_row
        bound = jnp.max(jnp.sum(jnp.abs(inner), axis=0, keepdims=True), axis=1, keepdims=True)
        x = eye - inner / bound
        both = jnp.where(left, z_gram, z) * (scale_column * lax.rsqrt(bound))
        x, total = lax.fori_loop(0, NS_ITERS - 1, polar_turn, (x, eye))
        both = dot(as_left(total), as_right(both))
        both = both + 0.5 * dot(as_left(x), as_right(both))
        other = pltpu.roll(both, size, 1)
        last = index == EIG_ITERS - 1
        return jnp.where(left == jnp.logical_not(last), both, other)

    return lax.fori_loop(0, EIG_ITERS, turn, gram)


def two_parts(values):
    high = values.astype(BF16)
    return high, (values - high.astype(F32)).astype(BF16)


def left_of_three(twice):
    rest = twice - twice.astype(BF16).astype(F32)
    first = jnp.where(left_mask(twice.shape), twice, rest).astype(BF16)
    return jnp.concatenate([first, twice.astype(BF16)], axis=1)[:, : 3 * twice.shape[1] // 2]


def right_of_three(values):
    high, low = two_parts(values)
    return jnp.concatenate([high, high, low], axis=0)


RAW = 2048
NEAR = 8
CORES = 2
TILE = 512
STATE = 16
VMEM = pl.BlockSpec(memory_space=pltpu.VMEM)
SMEM = pl.BlockSpec(memory_space=pltpu.SMEM)
ANY = pl.BlockSpec(memory_space=pl.ANY)
DMA = pltpu.SemaphoreType.DMA


def at_tile(index, start=0):
    return pl.ds(pl.multiple_of(start + index * TILE, 128), TILE)


def gram_terms(first, second):
    pieces = jnp.concatenate(two_parts(jnp.concatenate([first, second], axis=0)), axis=0)
    return lax.dot_general(pieces, pieces, NT, preferred_element_type=F32)


def step_kernel(
    distance, first_ref, second_ref, terms_ref, state_ref,
    stay_ref, come_ref, next_terms_ref, next_state_ref,
    grams, raw_first, raw_second, rows_out, rows_in, move_out, core_sums, near_sums, far_sums,
    core_send, core_recv,
    near_send, near_recv, far_send, far_recv, gram_send, gram_recv, raw_send, raw_recv, rows_send, rows_recv, move_send, move_recv,
):
    me = lax.axis_index("rows")
    count = lax.axis_size("rows")
    here = lax.axis_index("blk")
    cycle = lax.axis_size("blk")
    target = lax.rem(here + distance, cycle)
    origin = lax.rem(here + (cycle - distance), cycle)
    width, columns = first_ref.shape
    size = 2 * width
    wide = 2 * size
    tiles = (columns - RAW) // TILE

    core, near, far = lax.rem(here, CORES), lax.rem(here, NEAR) // CORES, here // NEAR
    line, groups = NEAR // CORES, cycle // NEAR

    def row_peer(away):
        return {"rows": lax.rem(me + away, count)}

    def near_peer(away):
        return {"blk": far * NEAR + lax.rem(near + away, line) * CORES + core}

    def core_peer(away):
        return {"blk": here + away - 2 * core}

    def far_peer(away):
        return {"blk": lax.rem(here + away * NEAR, cycle)}

    def each(peers, body):
        def one(away, carry):
            body(away)
            return carry

        lax.fori_loop(1, peers, one, 0)

    barrier = pltpu.get_barrier_semaphore()

    def greet(device):
        pl.semaphore_signal(barrier, inc=1, device_id=device, device_id_type=MESH)

    each(groups, lambda away: greet(far_peer(away)))
    each(count, lambda away: greet(row_peer(away)))
    greet({"blk": origin})
    greet(core_peer(1))
    each(line, lambda away: greet(near_peer(away)))

    def shared(buffer, slot, device, send_sem, recv_sem, away):
        return pltpu.make_async_remote_copy(
            src_ref=buffer.at[slot], dst_ref=buffer.at[slot],
            send_sem=send_sem.at[away - 1], recv_sem=recv_sem.at[away - 1],
            device_id=device, device_id_type=MESH,
        )

    def gram_copy(away):
        return shared(grams, me, row_peer(away), gram_send, gram_recv, away)

    def core_copy(away):
        return shared(core_sums, core, core_peer(away), core_send, core_recv, away)

    def near_copy(away):
        return shared(near_sums, near, near_peer(away), near_send, near_recv, away)

    def far_copy(away):
        return shared(far_sums, far, far_peer(away), far_send, far_recv, away)

    def to_target(source, destination, send_sem, recv_sem):
        return pltpu.make_async_remote_copy(
            src_ref=source, dst_ref=destination, send_sem=send_sem, recv_sem=recv_sem,
            device_id={"blk": target}, device_id_type=MESH,
        )

    end = pl.ds(columns - TILE, TILE)
    terms = terms_ref[...] + gram_terms(first_ref[:, end], second_ref[:, end])
    terms = terms[:size] + terms[size:]
    part = terms + pltpu.roll(terms, size, 1)
    left = left_mask((width, wide))
    grams[me] = jnp.where(left, part[:width], part[width:])

    pl.semaphore_wait(barrier, 1 + (count - 1) + (CORES - 1) + (line - 1) + (groups - 1))
    each(count, lambda away: gram_copy(away).start())
    raw = [
        to_target(first_ref.at[:, pl.ds(0, RAW)], raw_first, raw_send.at[0], raw_recv.at[0]),
        to_target(second_ref.at[:, pl.ds(0, RAW)], raw_second, raw_send.at[1], raw_recv.at[1]),
    ]
    for copy in raw:
        copy.start()
    each(count, lambda away: gram_copy(away).wait())
    packed = (grams[0] + grams[1]) + (grams[2] + grams[3])
    turned = pltpu.roll(packed, size, 1)
    gram = jnp.concatenate(
        [jnp.where(left, packed, turned), jnp.where(left, turned, packed)], axis=0
    )

    row = lax.broadcasted_iota(jnp.int32, gram.shape, 0)
    column = lax.broadcasted_iota(jnp.int32, gram.shape, 1)
    squares = jnp.where(column < size, gram * gram, 0.0)
    off = jnp.sum(jnp.where(column == row, 0.0, squares), axis=0, keepdims=True)
    diag = jnp.sum(jnp.where(column == row, squares, 0.0), axis=0, keepdims=True)
    core_sums[core] = jnp.concatenate([off, diag, jnp.zeros((6, wide), F32)], axis=0)
    core_copy(1).start()
    state = state_ref[...]
    flag = state[:1]

    def between(index):
        @pl.when(index == 1)
        def _():
            core_copy(1).wait()
            near_sums[near] = core_sums[0] + core_sums[1]
            each(line, lambda away: near_copy(away).start())

    rotation = rotation_rows(gram, between)
    top, bottom = rotation[:width], rotation[width:]
    staying = flag * bottom + (1.0 - flag) * top
    leaving = flag * top + (1.0 - flag) * bottom
    rows_out[...] = leaving
    rows_copy = to_target(rows_out, rows_in, rows_send, rows_recv)
    rows_copy.start()
    weights = left_of_three(jnp.concatenate([staying, leaving], axis=0))

    def move_copy(index):
        return to_target(
            move_out.at[:, at_tile(index)], come_ref.at[:, at_tile(index, RAW)],
            move_send.at[index], move_recv.at[index],
        )

    def rotate_tile(index, carry):
        tile = at_tile(index, RAW)
        current = jnp.concatenate([first_ref[:, tile], second_ref[:, tile]], axis=0)
        rotated = dot(weights, right_of_three(current))
        stay_ref[:, tile] = rotated[:width]
        move_out[:, at_tile(index)] = rotated[width:]

        @pl.when(index == tiles - 1)
        def _():
            each(line, lambda away: near_copy(away).wait())
            far_sums[far] = jnp.sum(near_sums[...], axis=0)
            each(groups, lambda away: far_copy(away).start())

        move_copy(index).start()
        return carry

    lax.fori_loop(0, tiles, rotate_tile, 0)

    for copy in raw:
        copy.wait()
    rows_copy.wait()
    arrived = left_of_three(rows_in[...])

    def come_tile(index, total):
        tile = at_tile(index)
        current = jnp.concatenate([first_ref[:, tile], second_ref[:, tile]], axis=0)
        other = jnp.concatenate([raw_first[:, tile], raw_second[:, tile]], axis=0)
        stay = dot(weights[:width], right_of_three(current))
        come = dot(arrived, right_of_three(other))
        stay_ref[:, tile] = stay
        come_ref[:, tile] = come
        return total + gram_terms(stay, come)

    total = lax.fori_loop(0, RAW // TILE, come_tile, jnp.zeros((wide, wide), F32))

    def wait_tile(index, total):
        move_copy(index).wait()
        tile = at_tile(index, RAW)
        return total + gram_terms(stay_ref[:, tile], come_ref[:, tile])

    next_terms_ref[...] = lax.fori_loop(0, tiles - 1, wait_tile, total)
    each(groups, lambda away: far_copy(away).wait())
    totals = jnp.sum(far_sums[...], axis=0)
    next_state_ref[...] = jnp.concatenate(
        [state[1 : STEPS + 1], flag, state[STEPS + 1 : 8], state[10:], totals[:2]], axis=0
    )
    move_copy(tiles - 1).wait()


def step(first, second, terms, state, distance):
    width, columns = first.shape
    block = jax.ShapeDtypeStruct((width, columns), F32)
    size = 2 * width
    tiles = (columns - RAW) // TILE
    return pl.pallas_call(
        partial(step_kernel, distance),
        out_shape=(
            block,
            block,
            jax.ShapeDtypeStruct((2 * size, 2 * size), F32),
            jax.ShapeDtypeStruct((STATE, 2 * size), F32),
        ),
        in_specs=[VMEM] * 4,
        out_specs=(VMEM,) * 4,
        scratch_shapes=[
            pltpu.VMEM((4, width, 2 * size), F32),
            pltpu.VMEM((width, RAW), F32),
            pltpu.VMEM((width, RAW), F32),
            pltpu.VMEM((width, 2 * size), F32),
            pltpu.VMEM((width, 2 * size), F32),
            pltpu.VMEM((width, columns - RAW), F32),
            pltpu.VMEM((CORES, 8, 2 * size), F32),
            pltpu.VMEM((NEAR // CORES, 8, 2 * size), F32),
            pltpu.VMEM((4, 8, 2 * size), F32),
            DMA((1,)), DMA((1,)), DMA((3,)), DMA((3,)), DMA((3,)), DMA((3,)),
            DMA((3,)), DMA((3,)), DMA((2,)), DMA((2,)), DMA, DMA, DMA((tiles,)), DMA((tiles,)),
        ],
        compiler_params=pltpu.CompilerParams(
            collective_id=distance, has_side_effects=True, vmem_limit_bytes=40 * 1024 * 1024
        ),
        name=f"step_{distance}",
    )(first, second, terms, state)


def begin_kernel(columns_ref, plan_any, first_ref, second_ref, terms_ref, state_ref, branch_any, plan_ref, branch_ref, sems):
    width, columns = first_ref.shape
    pieces = 2
    span = columns // pieces
    plan_copy = pltpu.make_async_copy(plan_any, plan_ref, sems.at[2 * pieces])
    plan_copy.start()
    copies = []
    for index in range(pieces):
        part = pl.ds(index * span, span)
        for half, block_ref in enumerate((first_ref, second_ref)):
            copy = pltpu.make_async_copy(
                columns_ref.at[pl.ds(half * width, width), part],
                block_ref.at[:, part],
                sems.at[2 * index + half],
            )
            copy.start()
            copies.append(copy)
    plan_copy.wait()
    rows = []
    slot = jnp.int32(0)
    for index in range(STEPS):
        stays = (plan_ref[index, 1] == 1).astype(jnp.int32)
        branch_ref[index] = jnp.maximum(plan_ref[index, 0] >> 1, plan_ref[index, 1] >> 1) - 1
        rows.append(jnp.full((1, 4 * width), ((1 - stays) == slot).astype(F32), F32))
        slot = stays
    rows.append(jnp.full((1, 4 * width), slot.astype(F32), F32))
    branch_copy = pltpu.make_async_copy(branch_ref, branch_any, sems.at[2 * pieces + 1])
    branch_copy.start()
    state_ref[...] = jnp.concatenate(rows + [jnp.zeros((STATE - STEPS - 1, 4 * width), F32)], axis=0)
    total = jnp.zeros((4 * width, 4 * width), F32)
    for index in range(pieces):
        copies[2 * index].wait()
        copies[2 * index + 1].wait()
        size = span if index < pieces - 1 else span - TILE
        part = pl.ds(index * span, size)
        total = total + gram_terms(first_ref[:, part], second_ref[:, part])
    terms_ref[...] = total
    branch_copy.wait()


def begin(columns, plan):
    width = columns.shape[0] // 2
    block = jax.ShapeDtypeStruct((width, columns.shape[1]), F32)
    return pl.pallas_call(
        begin_kernel,
        out_shape=(
            block,
            block,
            jax.ShapeDtypeStruct((4 * width, 4 * width), F32),
            jax.ShapeDtypeStruct((STATE, 4 * width), F32),
            jax.ShapeDtypeStruct((STEPS,), jnp.int32),
        ),
        in_specs=[ANY, ANY],
        out_specs=(VMEM,) * 4 + (ANY,),
        scratch_shapes=[
            pltpu.SMEM(plan.shape, jnp.int32), pltpu.SMEM((STEPS,), jnp.int32), DMA((10,)),
        ],
        name="begin",
    )(columns, plan)


def finish_kernel(first_ref, second_ref, state_ref, swept_ref, ratio_ref, ratios, sems):
    width = first_ref.shape[0]
    start = pl.multiple_of(state_ref[0, 0].astype(jnp.int32) * width, width)
    copies = [
        pltpu.make_async_copy(first_ref, swept_ref.at[pl.ds(start, width)], sems.at[0]),
        pltpu.make_async_copy(second_ref, swept_ref.at[pl.ds(width - start, width)], sems.at[1]),
    ]
    for copy in copies:
        copy.start()
    roots = jnp.sqrt(jnp.sum(state_ref[STATE - 8 :], axis=1, keepdims=True))
    for index in range(STEPS):
        row = 8 - 2 * (STEPS - index)
        ratios[index] = (roots[row : row + 1] / roots[row + 1 : row + 2])[0, 0]
    copies.append(pltpu.make_async_copy(ratios, ratio_ref, sems.at[2]))
    copies[-1].start()
    for copy in copies:
        copy.wait()


def finish(first, second, state):
    width, columns = first.shape
    return pl.pallas_call(
        finish_kernel,
        out_shape=(
            jax.ShapeDtypeStruct((2 * width, columns), F32),
            jax.ShapeDtypeStruct((STEPS,), F32),
        ),
        in_specs=[VMEM, VMEM, VMEM],
        out_specs=(ANY, ANY),
        scratch_shapes=[pltpu.SMEM((STEPS,), F32), DMA((3,))],
        name="finish",
    )(first, second, state)


def local(columns, plan):
    cycle = lax.axis_size("blk")
    branches = [partial(step, distance=distance) for distance in range(1, cycle)]
    *held, chosen = begin(columns, plan)

    def one_step(index, held):
        return tuple(lax.switch(chosen[index], branches, *held))

    first, second, terms, state = lax.fori_loop(0, STEPS, one_step, tuple(held))
    return tuple(finish(first, second, state))


def solution(mesh):
    return jax.shard_map(
        local,
        mesh=mesh,
        in_specs=(P("blk", "rows"), P()),
        out_specs=(P("blk", "rows"), P()),
        check_vma=False,
    )
```
